32 devices in a mesh: dp: 8 (over z, x), tensor: 4 (over y, core).
Axes of the slice: x: 2, y: 2, z: 4, core: 2. Of those that a mesh axis runs over, the one named last changes fastest.
Arguments:
- hidden: bfloat16 [2048, 14336], P('dp', 'tensor'), parts along dimension 0, may hold values from -16 to 16
- signs: int32 [14336], P('tensor'), may hold values 0 or 1
- packed: int32 [14336, 512], P('tensor'), may hold values from -2147483648 to 2147483646
- group_scales: int32 [112, 4096], P('tensor'), may hold values from 1 to 16
- residual: bfloat16 [2048, 4096], P(('dp', 'tensor')), parts along dimension 0, may hold values from -16 to 16
Outputs:
- new_residual: bfloat16 [2048, 4096], P(('dp', 'tensor')), parts along dimension 0
- normed: bfloat16 [2048, 4096], P(('dp', 'tensor')), parts along dimension 0
The draws below stay inside these ranges and needn't reach their ends.
There are 8 independent parts, one for each index of `dp`. The reference program is written for one: setup_inputs(seed, part) draws one part's arguments, and reference() takes and returns one part's arrays. A program takes and returns all parts, laid end to end along the dimension named above; an argument that names none is the same for every part. Nothing has to cross between parts.
Inputs may be any that keep to these rules, and one draw needn't show every extreme that they name: `packed`: bits 4 k to 4 k + 3 of word j in row f hold the code of output feature k * 512 + j plus 8.
All inputs are finite; a program needn't handle non-finite values. No bound on the sum of `signs` on one device may be relied on, other than what follows from the above.
Results may differ from the reference program's by a relative error of at most 0.0054.
Values may be sent and summed in bfloat16 or wider, within the bound.
No kernel may reach another device: no remote copies, remote signals or barrier semaphores. Data moves between devices by JAX's collectives and lax.ppermute only.
A program may use at most 256 MiB of HBM per device.

```python
import math
import jax
import jax.numpy as jnp
import numpy as np
from jax import lax

D = 4096
FF = 14336
GROUP = 128
ROWS = 256


def scaled_draw(key, count, width):
    first = jax.random.fold_in(key, 0)
    third = jax.random.fold_in(key, 2)
    column_scale = jnp.exp(jax.random.uniform(first, (1, width), jnp.float32, math.log(0.3), math.log(3.0)))
    values = jax.random.normal(third, (count, width), jnp.float32) * column_scale
    return jnp.clip(values, -16.0, 16.0)


def draw_hidden(key, part):
    return scaled_draw(jax.random.fold_in(key, 11), ROWS, FF).astype(jnp.bfloat16)


def draw_residual(key, part):
    return scaled_draw(jax.random.fold_in(key, 23), ROWS, D).astype(jnp.bfloat16)


def touch_ends(values, rng, low, high):
    spot = [jax.random.randint(jax.random.fold_in(rng, axis), (), 0, length) for axis, length in enumerate(values.shape)]
    main_axis = values.shape.index(max(values.shape))
    beside = spot[:main_axis] + [(spot[main_axis] + 1) % values.shape[main_axis]] + spot[main_axis + 1:]
    return values.at[tuple(spot)].set(low).at[tuple(beside)].set(high)


def setup_inputs(seed: int = 0, part: int = 0) -> dict:
    key_of = jax.random.split(jax.random.key(seed), 6)
    own_keys = jax.random.split(jax.random.fold_in(key_of[5], part), 6)
    hidden = draw_hidden(jax.random.fold_in(jax.random.fold_in(key_of[5], part), 71), part)
    signs = touch_ends((jax.random.randint(key_of[1], (FF,), 0, 2) < 1).astype(jnp.int32), jax.random.fold_in(key_of[1], 1), 0, 1)
    packed = touch_ends(jax.random.randint(key_of[2], (FF, D // 8), -2147483648, 2147483647), jax.random.fold_in(key_of[2], 1), -2147483648, 2147483646).astype(jnp.int32)
    group_scales = touch_ends(jax.random.randint(key_of[3], (FF // GROUP, D), 1, 17), jax.random.fold_in(key_of[3], 1), 1, 16).astype(jnp.int32)
    residual = draw_residual(jax.random.fold_in(jax.random.fold_in(key_of[5], part), 71), part)
    return {"hidden": hidden, "signs": signs, "packed": packed, "group_scales": group_scales, "residual": residual}


def paley_table():
    offsets = (np.arange(13)[None, :] - np.arange(13)[:, None]) % 13
    residues = np.zeros(13)
    residues[np.arange(1, 13) ** 2 % 13] = 1.0
    quadratic = np.where(offsets == 0, 0.0, np.where(residues[offsets] > 0, 1.0, -1.0))
    conference = np.zeros((14, 14))
    conference[0, 1:] = 1.0
    conference[1:, 0] = 1.0
    conference[1:, 1:] = quadratic
    upper = np.array([[1.0, 1.0], [1.0, -1.0]])
    lower = np.array([[1.0, -1.0], [-1.0, -1.0]])
    return np.kron(conference, upper) + np.kron(np.eye(14), lower)

def sylvester(order):
    first = lax.broadcasted_iota(jnp.int32, (order, order), 0)
    second = lax.broadcasted_iota(jnp.int32, (order, order), 1)
    common = first & second
    parity = jnp.zeros((order, order), jnp.int32)
    for bit in range(max(order.bit_length() - 1, 0)):
        parity = parity ^ jnp.right_shift(common, bit) & 1
    return (1 - 2 * parity).astype(jnp.float32)

def reference(hidden, signs, packed, group_scales, residual):
    count = hidden.shape[0]
    flips = (2 * signs - 1).astype(jnp.float32)
    signed = hidden.astype(jnp.float32) * flips[None, :]
    blocks = signed.reshape(count, FF // 28, 28)
    outer = sylvester(FF // 28)
    inner = jnp.asarray(paley_table(), jnp.float32)
    mixed = jnp.einsum('rba,cb->rca', blocks, outer, precision=lax.Precision.HIGHEST)
    mixed = jnp.einsum('rca,da->rcd', mixed, inner, precision=lax.Precision.HIGHEST)
    rotated = (mixed.reshape(count, FF) * (1.0 / math.sqrt(FF))).astype(jnp.bfloat16)
    width = D // 8
    pieces = []
    for nibble in range(8):
        codes = (jnp.right_shift(packed, 4 * nibble) & 15) - 8
        scales = group_scales[:, nibble * width:(nibble + 1) * width]
        weights = (codes.reshape(FF // GROUP, GROUP, width) * scales[:, None, :]).reshape(FF, width)
        pieces.append(jnp.dot(rotated, weights.astype(jnp.bfloat16), preferred_element_type=jnp.float32))
    branch = jnp.concatenate(pieces, axis=1) * (1.0 / (45.0 * math.sqrt(FF)))
    new_residual = (residual.astype(jnp.float32) + branch).astype(jnp.bfloat16)
    values = new_residual.astype(jnp.float32)
    normed = values * lax.rsqrt(lax.optimization_barrier(jnp.mean(values * values, axis=1, keepdims=True)) + 1e-05)
    return (new_residual, normed.astype(jnp.bfloat16))
```

```python
import functools
import math

import jax
import jax.numpy as jnp
import numpy as np
from jax import lax
from jax.experimental import pallas as pl
from jax.experimental.pallas import tpu as pltpu
from jax.sharding import PartitionSpec as P

ORDER = 28
DENSE = 896
TILE_ROWS = 16
COLUMN_TILE = 512


def paley_table():
    offsets = (np.arange(13)[None, :] - np.arange(13)[:, None]) % 13
    residues = np.zeros(13)
    residues[np.arange(1, 13) ** 2 % 13] = 1.0
    quadratic = np.where(offsets == 0, 0.0, np.where(residues[offsets] > 0, 1.0, -1.0))
    conference = np.zeros((14, 14))
    conference[0, 1:] = 1.0
    conference[1:, 0] = 1.0
    conference[1:, 1:] = quadratic
    upper = np.array([[1.0, 1.0], [1.0, -1.0]])
    lower = np.array([[1.0, -1.0], [-1.0, -1.0]])
    return np.kron(conference, upper) + np.kron(np.eye(14), lower)


def sylvester(order):
    table = np.ones((1, 1))
    while table.shape[0] < order:
        table = np.kron(np.array([[1.0, 1.0], [1.0, -1.0]]), table)
    return table


def dense_table():
    return np.kron(sylvester(DENSE // ORDER), paley_table().T)


def dequantize_kernel(packed_ref, scales_ref, weights_ref):
    group_count = scales_ref.shape[0]
    group_size = packed_ref.shape[0] // group_count
    words = packed_ref.shape[1]

    @pl.loop(0, group_count)
    def _(group):
        rows = pl.ds(pl.multiple_of(group * group_size, group_size), group_size)
        word = packed_ref[rows, :] ^ np.int32(-2004318072)
        for nibble in range(8):
            columns = pl.ds(nibble * words, words)
            codes = jnp.right_shift(jnp.left_shift(word, 28 - 4 * nibble), 28)
            scale = scales_ref[pl.ds(group, 1), columns].astype(jnp.float32)
            weights_ref[rows, columns] = (codes.astype(jnp.float32) * scale).astype(jnp.bfloat16)


def dequantize(packed, group_scales):
    width, words = packed.shape
    return pl.pallas_call(
        dequantize_kernel,
        out_shape=pltpu.VMEM((width, 8 * words), jnp.bfloat16),
        in_specs=[pl.BlockSpec(memory_space=pltpu.VMEM)] * 2,
        out_specs=pl.BlockSpec(memory_space=pltpu.VMEM),
        compiler_params=pltpu.CompilerParams(vmem_limit_bytes=24 * 2**20),
        cost_estimate=pl.CostEstimate(
            flops=width * words * 8 * 4, bytes_accessed=width * words * 4, transcendentals=0
        ),
        name="dequantize",
    )(packed, group_scales)


def project_kernel(groups, unit, coef_ref, core_ref, *refs):
    parts = refs[:groups]
    table_ref, weights_ref, keep_ref, send_ref, rotated_ref = refs[groups:]
    rows, width = parts[0].shape
    blocks = width // DENSE
    mixed = []
    for block in range(blocks):
        columns = pl.ds(block * DENSE, DENSE)
        total = coef_ref[0] * parts[0][:, columns].astype(jnp.float32)
        for r in range(1, groups):
            total = total + coef_ref[r] * parts[r][:, columns].astype(jnp.float32)
        mixed.append(total)
    span = 1
    while span < blocks:
        for first in range(blocks):
            if not first & span:
                a, b = mixed[first], mixed[first + span]
                mixed[first], mixed[first + span] = a + b, a - b
        span *= 2
    for block in range(blocks):
        high = mixed[block].astype(jnp.bfloat16)
        low = (mixed[block] - high.astype(jnp.float32)).astype(jnp.bfloat16)
        both = jnp.dot(
            jnp.concatenate([high, low], axis=0), table_ref[...], preferred_element_type=jnp.float32
        )
        rotated_ref[:, pl.ds(block * DENSE, DENSE)] = (
            (both[:rows] + both[rows:]) * unit
        ).astype(jnp.bfloat16)
    half = rows // 2
    upper = core_ref[0] == 1

    @pl.loop(0, weights_ref.shape[1] // COLUMN_TILE)
    def _(tile):
        columns = pl.ds(pl.multiple_of(tile * COLUMN_TILE, COLUMN_TILE), COLUMN_TILE)
        product = jnp.dot(
            rotated_ref[...], weights_ref[:, columns], preferred_element_type=jnp.float32
        )
        first, second = product[:half], product[half:]
        keep_ref[:, columns] = jnp.where(upper, second, first)
        send_ref[:, columns] = jnp.where(upper, first, second).astype(jnp.bfloat16)


def project(parts, coef, core, table, weights, unit):
    groups = len(parts)
    rows, width = parts[0].shape
    features = weights.shape[1]
    vmem = pl.BlockSpec(memory_space=pltpu.VMEM)
    smem = pl.BlockSpec(memory_space=pltpu.SMEM)
    return pl.pallas_call(
        functools.partial(project_kernel, groups, unit),
        out_shape=(
            jax.ShapeDtypeStruct((rows // 2, features), jnp.float32),
            jax.ShapeDtypeStruct((rows // 2, features), jnp.bfloat16),
        ),
        in_specs=[smem, smem] + [vmem] * (groups + 2),
        out_specs=(vmem, vmem),
        scratch_shapes=[pltpu.VMEM((rows, width), jnp.bfloat16)],
        compiler_params=pltpu.CompilerParams(vmem_limit_bytes=24 * 2**20),
        cost_estimate=pl.CostEstimate(
            flops=2 * rows * width * (features + 2 * DENSE),
            bytes_accessed=2 * groups * rows * width,
            transcendentals=0,
        ),
        name="project",
    )(coef, core, *parts, table, pltpu.with_memory_space_constraint(weights, pltpu.VMEM))


def local(hidden, signs, packed, group_scales, residual):
    groups = lax.axis_size("tensor")
    bits = groups.bit_length() - 1
    me = lax.axis_index("tensor")
    width = hidden.shape[1]
    total_width = width * groups
    token_rows = residual.shape[0]
    chunks = token_rows // TILE_ROWS
    features = residual.shape[1]
    unit = 1.0 / math.sqrt(total_width)
    flips = (2 * signs - 1).astype(jnp.bfloat16)

    def swap(value, bit):
        return lax.ppermute(value, "tensor", [(i, i ^ (1 << bit)) for i in range(groups)])

    relative = jnp.arange(groups, dtype=jnp.int32)
    common = me & (me ^ relative)
    parity = jnp.zeros_like(common)
    for bit in range(bits):
        parity = parity ^ (jnp.right_shift(common, bit) & 1)
    coef = (1 - 2 * parity).astype(jnp.float32)
    core = (me & 1).reshape(1)

    by_rows = hidden.reshape((2,) * bits + (chunks, TILE_ROWS, width))
    own = []
    for chunk in range(chunks):
        piece = lax.index_in_dim(by_rows, chunk, axis=bits, keepdims=False)
        piece = jnp.transpose(piece, tuple(reversed(range(bits))) + (bits, bits + 1))
        own.append(piece.reshape(groups * TILE_ROWS, width) * flips[None, :])
    gathered = []
    for chunk in range(chunks):
        have = {0: own[chunk]}
        for bit in reversed(range(bits)):
            have.update({r ^ (1 << bit): swap(value, bit) for r, value in list(have.items())})
        gathered.append([have[r] for r in range(groups)])
    table = jnp.asarray(dense_table(), jnp.bfloat16)
    weights = dequantize(packed, group_scales)
    out_new, out_normed = [], []
    for chunk in range(chunks):
        value, send = project(gathered[chunk], coef, core, table, weights, unit)
        value = value + swap(send, 0).astype(jnp.float32)
        for bit in range(1, bits):
            half = value.shape[0] // 2
            upper = (jnp.right_shift(me, bit) & 1) == 1
            send = jnp.where(upper, value[:half], value[half:]).astype(jnp.bfloat16)
            value = jnp.where(upper, value[half:], value[:half]) + swap(send, bit).astype(jnp.float32)
        branch = value * (1.0 / (45.0 * math.sqrt(total_width)))
        start = residual[chunk * TILE_ROWS : (chunk + 1) * TILE_ROWS].astype(jnp.float32)
        new_residual = (start + branch).astype(jnp.bfloat16)
        values = new_residual.astype(jnp.float32)
        normed = values * lax.rsqrt(jnp.mean(values * values, axis=1, keepdims=True) + 1e-05)
        out_new.append(new_residual)
        out_normed.append(normed.astype(jnp.bfloat16))
    return jnp.concatenate(out_new, axis=0), jnp.concatenate(out_normed, axis=0)


def solution(mesh):
    return jax.shard_map(
        local,
        mesh=mesh,
        in_specs=(
            P("dp", "tensor"),
            P("tensor"),
            P("tensor", None),
            P("tensor", None),
            P(("dp", "tensor"), None),
        ),
        out_specs=(P(("dp", "tensor"), None), P(("dp", "tensor"), None)),
        check_vma=False,
    )
```

```python
import functools
import math

import jax
import jax.numpy as jnp
import numpy as np
from jax import lax
from jax.experimental import pallas as pl
from jax.experimental.pallas import tpu as pltpu
from jax.sharding import PartitionSpec as P


ORDER = 28
DENSE = 896
TILE_ROWS = 16
VMEM = pl.BlockSpec(memory_space=pltpu.VMEM)
SMEM = pl.BlockSpec(memory_space=pltpu.SMEM)
HBM = pl.BlockSpec(memory_space=pltpu.HBM)
NIBBLES = 8


def chunk_rows(token_rows):
    quarter = token_rows // 4
    if quarter % TILE_ROWS:
        return [token_rows]
    return [quarter, 2 * quarter, quarter]


def paley_table():
    offsets = (np.arange(13)[None, :] - np.arange(13)[:, None]) % 13
    residues = np.zeros(13)
    residues[np.arange(1, 13) ** 2 % 13] = 1.0
    quadratic = np.where(offsets == 0, 0.0, np.where(residues[offsets] > 0, 1.0, -1.0))
    conference = np.zeros((14, 14))
    conference[0, 1:] = 1.0
    conference[1:, 0] = 1.0
    conference[1:, 1:] = quadratic
    upper = np.array([[1.0, 1.0], [1.0, -1.0]])
    lower = np.array([[1.0, -1.0], [-1.0, -1.0]])
    return np.kron(conference, upper) + np.kron(np.eye(14), lower)


def sylvester(order):
    table = np.ones((1, 1))
    while table.shape[0] < order:
        table = np.kron(np.array([[1.0, 1.0], [1.0, -1.0]]), table)
    return table


def cost(flops):
    return pl.CostEstimate(flops=flops, bytes_accessed=0, transcendentals=0)


def dense_table():
    return np.kron(sylvester(DENSE // ORDER), paley_table().T)


def bit_reversed(groups):
    bits = groups.bit_length() - 1
    return [sum(((d >> b) & 1) << (bits - 1 - b) for b in range(bits)) for d in range(groups)]


def sign_of(bit):
    return (1 - 2 * bit).astype(jnp.float32)


def prepare_kernel(groups, sizes, hidden_ref, signs_ref, first_ref, *rest_ref):
    token_rows = sum(sizes)
    flips = (2 * signs_ref[...] - 1).astype(jnp.float32)
    at, start = 0, 0
    for chunk, size in enumerate(sizes):
        for owner in bit_reversed(groups):
            rows = hidden_ref[pl.ds(owner * token_rows + start, size), :]
            value = (rows.astype(jnp.float32) * flips).astype(jnp.bfloat16)
            if chunk == 0:
                first_ref[pl.ds(at, size), :] = value
            else:
                rest_ref[0][pl.ds(at - groups * sizes[0], size), :] = value
            at += size
        start += size


def prepare(hidden, signs, groups, sizes):
    rows, width = hidden.shape
    size = groups * sizes[0]
    shapes = [jax.ShapeDtypeStruct((size, width), jnp.bfloat16)]
    if len(sizes) > 1:
        shapes.append(jax.ShapeDtypeStruct((rows - size, width), jnp.bfloat16))
    return pl.pallas_call(
        functools.partial(prepare_kernel, groups, sizes),
        out_shape=shapes,
        in_specs=[VMEM, VMEM],
        out_specs=[VMEM] * len(shapes),
        compiler_params=pltpu.CompilerParams(vmem_limit_bytes=12 * 2**20),
        cost_estimate=cost(rows * width),
        name="prepare",
    )(hidden, signs.reshape(1, width))


def rotate_blocks(mixed, table_ref):
    rows = mixed[0].shape[0]
    blocks = len(mixed)
    span = 1
    while span < blocks:
        for first in range(blocks):
            if not first & span:
                a, b = mixed[first], mixed[first + span]
                mixed[first], mixed[first + span] = a + b, a - b
        span *= 2
    out = []
    for block in range(blocks):
        high = mixed[block].astype(jnp.bfloat16)
        low = (mixed[block] - high.astype(jnp.float32)).astype(jnp.bfloat16)
        both = jnp.dot(
            jnp.concatenate([high, low], axis=0), table_ref[...], preferred_element_type=jnp.float32
        )
        out.append(both[:rows] + both[rows:])
    return out


def rotate_kernel(sizes, me_ref, own_ref, other_ref, table_ref, *out_refs):
    blocks = own_ref.shape[1] // DENSE
    sign = sign_of(me_ref[0] & 1)
    start = 0
    for chunk, size in enumerate(sizes):
        at = pl.ds(start, size)
        start += size
        mixed = []
        for block in range(blocks):
            columns = pl.ds(block * DENSE, DENSE)
            mixed.append(
                sign * own_ref[at, columns].astype(jnp.float32)
                + other_ref[at, columns].astype(jnp.float32)
            )
        for block, value in enumerate(rotate_blocks(mixed, table_ref)):
            columns = pl.ds(block * DENSE, DENSE)
            out_refs[2 * chunk][:, columns] = value
            out_refs[2 * chunk + 1][:, columns] = value.astype(jnp.bfloat16)


def rotate(own, other, me, table, sizes):
    rows, width = own.shape
    shapes = []
    for size in sizes:
        shapes.append(jax.ShapeDtypeStruct((size, width), jnp.float32))
        shapes.append(jax.ShapeDtypeStruct((size, width), jnp.bfloat16))
    return pl.pallas_call(
        functools.partial(rotate_kernel, sizes),
        out_shape=shapes,
        in_specs=[SMEM, VMEM, VMEM, VMEM],
        out_specs=[VMEM] * len(shapes),
        compiler_params=pltpu.CompilerParams(vmem_limit_bytes=20 * 2**20),
        cost_estimate=cost(4 * rows * width * DENSE),
        name="rotate",
    )(me, own, other, table)


def dequantize_kernel(group_size, packed_ref, scales_ref, weights_ref):
    words = packed_ref.shape[1]
    share = packed_ref.shape[0] // group_size
    for part in range(share):
        group = pl.program_id(0) * share + part
        rows = pl.ds(part * group_size, group_size)
        word = packed_ref[rows, :] ^ np.int32(-2004318072)
        for nibble in range(NIBBLES):
            codes = jnp.right_shift(jnp.left_shift(word, 28 - 4 * nibble), 28)
            scale = scales_ref[pl.ds(group, 1), pl.ds(nibble * words, words)]
            weights_ref[nibble, rows, :] = (codes * scale).astype(jnp.int8)


def dequantize(packed, group_scales):
    width, words = packed.shape
    group_count = group_scales.shape[0]
    group_size = width // group_count
    rows = group_size * (2 - group_count % 2)
    return pl.pallas_call(
        functools.partial(dequantize_kernel, group_size),
        grid=(width // rows,),
        out_shape=pltpu.HBM((NIBBLES, width, words), jnp.int8),
        in_specs=[
            pl.BlockSpec((rows, words), lambda i: (i, 0)),
            pl.BlockSpec(group_scales.shape, lambda i: (0, 0)),
        ],
        out_specs=pl.BlockSpec((NIBBLES, rows, words), lambda i: (0, i, 0)),
        compiler_params=pltpu.CompilerParams(vmem_limit_bytes=12 * 2**20),
        cost_estimate=cost(width * words * 8 * 1024),
        name="dequantize",
    )(packed, group_scales)


def project_kernel(count, unit, rotate_first, me_ref, *refs):
    parts = refs[:count]
    refs = refs[count:]
    if rotate_first:
        table_ref, refs = refs[0], refs[1:]
    weights_ref, keep_ref, send_ref, rotated_ref, buffer, sems = refs
    fetches = [
        pltpu.make_async_copy(weights_ref.at[n], buffer.at[n], sems.at[n]) for n in range(NIBBLES)
    ]
    for fetch in fetches:
        fetch.start()
    rows, width = parts[0].shape
    words = weights_ref.shape[2]
    blocks = width // DENSE
    me = me_ref[0]
    signs = []
    for r in range(count):
        bits = me & (me ^ r) if rotate_first else jnp.right_shift(me, 1) & (1 - r)
        parity = bits & 1
        for shift in range(1, max(count.bit_length() - 1, 1)):
            parity = parity ^ (jnp.right_shift(bits, shift) & 1)
        signs.append(sign_of(parity))
    mixed = []
    for block in range(blocks):
        columns = pl.ds(block * DENSE, DENSE)
        total = signs[0] * parts[0][:, columns].astype(jnp.float32)
        for r in range(1, count):
            total = total + signs[r] * parts[r][:, columns].astype(jnp.float32)
        mixed.append(total)
    if rotate_first:
        mixed = rotate_blocks(mixed, table_ref)
    for block in range(blocks):
        rotated_ref[:, pl.ds(block * DENSE, DENSE)] = (mixed[block] * unit).astype(jnp.bfloat16)
    half = rows // 2
    upper = me & 1 == 1

    @pl.loop(0, NIBBLES)
    def _(nibble):
        pltpu.make_async_copy(weights_ref.at[nibble], buffer.at[nibble], sems.at[nibble]).wait()
        product = jnp.dot(
            rotated_ref[...],
            buffer[nibble].astype(jnp.bfloat16),
            preferred_element_type=jnp.float32,
        )
        first, second = product[:half], product[half:]
        columns = pl.ds(pl.multiple_of(nibble * words, words), words)
        keep_ref[:, columns] = jnp.where(upper, second, first)
        send_ref[:, columns] = jnp.where(upper, first, second).astype(jnp.bfloat16)


def project(parts, me, table, weights, unit):
    count = len(parts)
    rows, width = parts[0].shape
    words = weights.shape[2]
    features = NIBBLES * words
    tables = [] if table is None else [table]
    return pl.pallas_call(
        functools.partial(project_kernel, count, unit, table is not None),
        out_shape=(
            jax.ShapeDtypeStruct((rows // 2, features), jnp.float32),
            jax.ShapeDtypeStruct((rows // 2, features), jnp.bfloat16),
        ),
        in_specs=[SMEM] + [VMEM] * (count + len(tables)) + [HBM],
        out_specs=(VMEM, VMEM),
        scratch_shapes=[
            pltpu.VMEM((rows, width), jnp.bfloat16),
            pltpu.VMEM(weights.shape, jnp.int8),
            pltpu.SemaphoreType.DMA((NIBBLES,)),
        ],
        compiler_params=pltpu.CompilerParams(vmem_limit_bytes=28 * 2**20),
        cost_estimate=cost(2 * 128 * width * features),
        name="project",
    )(me, *parts, *tables, pltpu.with_memory_space_constraint(weights, pltpu.HBM))


def finish_kernel(sizes, scale, *refs):
    chunks = len(sizes)
    keeps, gots = refs[:chunks], refs[chunks : 2 * chunks]
    residual_ref, new_ref, normed_ref = refs[2 * chunks :]
    start = 0
    for chunk, size in enumerate(sizes):
        rows = pl.ds(start, size)
        start += size
        branch = (keeps[chunk][...] + gots[chunk][...].astype(jnp.float32)) * scale
        fresh = (residual_ref[rows, :].astype(jnp.float32) + branch).astype(jnp.bfloat16)
        new_ref[rows, :] = fresh
        values = fresh.astype(jnp.float32)
        inverse = lax.rsqrt(jnp.mean(values * values, axis=1, keepdims=True) + 1e-05)
        normed_ref[rows, :] = (values * inverse).astype(jnp.bfloat16)


def finish(keeps, gots, residual, scale):
    chunks = len(keeps)
    shape = jax.ShapeDtypeStruct(residual.shape, jnp.bfloat16)
    return pl.pallas_call(
        functools.partial(finish_kernel, [keep.shape[0] for keep in keeps], scale),
        out_shape=(shape, shape),
        in_specs=[VMEM] * (2 * chunks + 1),
        out_specs=(VMEM, VMEM),
        compiler_params=pltpu.CompilerParams(vmem_limit_bytes=12 * 2**20),
        cost_estimate=cost(residual.size * 1024),
        name="finish",
    )(*keeps, *gots, residual)


def local(hidden, signs, packed, group_scales, residual):
    groups = lax.axis_size("tensor")
    bits = groups.bit_length() - 1
    me = lax.axis_index("tensor")
    where = me.reshape(1)
    total_width = hidden.shape[1] * groups
    sizes = chunk_rows(residual.shape[0])
    chunks = len(sizes)
    unit = 1.0 / math.sqrt(total_width)
    table = jnp.asarray(dense_table(), jnp.bfloat16)

    def swap(value, bit):
        return lax.ppermute(value, "tensor", [(i, i ^ (1 << bit)) for i in range(groups)])

    def bit_of(bit):
        return jnp.right_shift(me, bit) & 1

    own = prepare(hidden, signs, groups, sizes)
    have = {0: own[0]}
    for bit in reversed(range(bits)):
        have.update({r ^ (1 << bit): swap(value, bit) for r, value in list(have.items())})
    stages = [([have[r] for r in range(groups)], table)]
    if chunks > 1:
        other = swap(own[1], 0)
        pairs = rotate(own[1], other, where, table, [groups * size for size in sizes[1:]])
        for chunk in range(1, chunks):
            keep, send = pairs[2 * chunk - 2], pairs[2 * chunk - 1]
            for bit in range(1, bits):
                got = swap(send, bit)
                if bit < bits - 1:
                    keep = sign_of(bit_of(bit)) * keep + got.astype(jnp.float32)
                    send = keep.astype(jnp.bfloat16)
            stages.append(([keep, got], None))
    weights = dequantize(packed, group_scales)
    keeps, gots = [], []
    for parts, maybe_table in stages:
        value, send = project(parts, where, maybe_table, weights, unit)
        got = swap(send, 0)
        for bit in range(1, bits):
            value = value + got.astype(jnp.float32)
            half = value.shape[0] // 2
            upper = bit_of(bit) == 1
            send = jnp.where(upper, value[:half], value[half:]).astype(jnp.bfloat16)
            value = jnp.where(upper, value[half:], value[:half])
            got = swap(send, bit)
        keeps.append(value)
        gots.append(got)
    return finish(keeps, gots, residual, 1.0 / (45.0 * math.sqrt(total_width)))


def solution(mesh):
    return jax.shard_map(
        local,
        mesh=mesh,
        in_specs=(
            P("dp", "tensor"),
            P("tensor"),
            P("tensor", None),
            P("tensor", None),
            P(("dp", "tensor"), None),
        ),
        out_specs=(P(("dp", "tensor"), None), P(("dp", "tensor"), None)),
        check_vma=False,
    )
```

```python
import functools
import math

import jax
import jax.numpy as jnp
import numpy as np
from jax import lax
from jax.experimental import pallas as pl
from jax.experimental.pallas import tpu as pltpu
from jax.sharding import PartitionSpec as P


ORDER = 28
DENSE = 896
TILE_ROWS = 16
VMEM = pl.BlockSpec(memory_space=pltpu.VMEM)
SMEM = pl.BlockSpec(memory_space=pltpu.SMEM)
HBM = pl.BlockSpec(memory_space=pltpu.HBM)
ANY = pl.BlockSpec(memory_space=pl.ANY)
NIBBLES = 8


def chunk_rows(token_rows):
    quarter = token_rows // 4
    if quarter % TILE_ROWS:
        return [token_rows]
    return [quarter, 2 * quarter, quarter]


def paley_table():
    offsets = (np.arange(13)[None, :] - np.arange(13)[:, None]) % 13
    residues = np.zeros(13)
    residues[np.arange(1, 13) ** 2 % 13] = 1.0
    quadratic = np.where(offsets == 0, 0.0, np.where(residues[offsets] > 0, 1.0, -1.0))
    conference = np.zeros((14, 14))
    conference[0, 1:] = 1.0
    conference[1:, 0] = 1.0
    conference[1:, 1:] = quadratic
    upper = np.array([[1.0, 1.0], [1.0, -1.0]])
    lower = np.array([[1.0, -1.0], [-1.0, -1.0]])
    return np.kron(conference, upper) + np.kron(np.eye(14), lower)


def sylvester(order):
    table = np.ones((1, 1))
    while table.shape[0] < order:
        table = np.kron(np.array([[1.0, 1.0], [1.0, -1.0]]), table)
    return table


def cost(flops):
    return pl.CostEstimate(flops=flops, bytes_accessed=0, transcendentals=0)


def dense_table():
    return np.kron(sylvester(DENSE // ORDER), paley_table().T)


def bit_reversed(groups):
    bits = groups.bit_length() - 1
    return [sum(((d >> b) & 1) << (bits - 1 - b) for b in range(bits)) for d in range(groups)]


def sign_of(bit):
    return (1 - 2 * bit).astype(jnp.float32)


def prepare_kernel(groups, token_rows, places, hidden_ref, signs_ref, *refs):
    out_refs, (staged, sems) = refs[:-2], refs[-2:]
    width = hidden_ref.shape[1]
    copies, at = [], 0
    for start, size in places:
        for owner in bit_reversed(groups):
            copies.append(
                pltpu.make_async_copy(
                    hidden_ref.at[pl.ds(owner * token_rows + start, size), :],
                    staged.at[pl.ds(at, size), :],
                    sems.at[len(copies)],
                )
            )
            copies[-1].start()
            at += size
    flips = (2 * signs_ref[...] - 1).astype(jnp.float32).reshape(1, width)
    at = 0
    for index, copy in enumerate(copies):
        size = places[index // groups][1]
        copy.wait()
        rows = pl.ds(at, size)
        value = (staged[rows, :].astype(jnp.float32) * flips).astype(jnp.bfloat16)
        for out_ref in out_refs:
            out_ref[rows, :] = value
        at += size


def prepare(hidden, signs, groups, places, outputs):
    width = hidden.shape[1]
    rows = groups * sum(size for _, size in places)
    count = groups * len(places)
    return pl.pallas_call(
        functools.partial(prepare_kernel, groups, hidden.shape[0] // groups, places),
        out_shape=[jax.ShapeDtypeStruct((rows, width), jnp.bfloat16)]
        + [pltpu.HBM((rows, width), jnp.bfloat16)] * (outputs - 1),
        in_specs=[HBM, VMEM],
        out_specs=[VMEM] * outputs,
        scratch_shapes=[
            pltpu.VMEM((rows, width), jnp.bfloat16),
            pltpu.SemaphoreType.DMA((count,)),
        ],
        compiler_params=pltpu.CompilerParams(vmem_limit_bytes=12 * 2**20),
        cost_estimate=cost(rows * width),
        name="prepare",
    )(pltpu.with_memory_space_constraint(hidden, pltpu.HBM), signs)


def rotate_blocks(mixed, table_ref, stacked_ref):
    rows = mixed[0].shape[0]
    blocks = len(mixed)
    span = 1
    while span < blocks:
        for first in range(blocks):
            if not first & span:
                a, b = mixed[first], mixed[first + span]
                mixed[first], mixed[first + span] = a + b, a - b
        span *= 2
    for block in range(blocks):
        stacked_ref[pl.ds(block * rows, rows), :] = mixed[block].astype(jnp.bfloat16)
    turned = jnp.dot(stacked_ref[...], table_ref[...], preferred_element_type=jnp.float32)
    return [turned[block * rows : (block + 1) * rows] for block in range(blocks)]


def rotate_kernel(sizes, me_ref, own_in, other_in, table_in, *refs):
    out_refs, stacked_ref = refs[:-5], refs[-5]
    own_ref, other_ref, table_ref, sems = refs[-4:]
    moves = [
        pltpu.make_async_copy(own_in, own_ref, sems.at[0]),
        pltpu.make_async_copy(other_in, other_ref, sems.at[1]),
        pltpu.make_async_copy(table_in, table_ref, sems.at[2]),
    ]
    for move in moves:
        move.start()
    for move in moves:
        move.wait()
    blocks = own_ref.shape[1] // DENSE
    sign = sign_of(me_ref[0] & 1)
    mixed = []
    for block in range(blocks):
        columns = pl.ds(block * DENSE, DENSE)
        mixed.append(
            sign * own_ref[:, columns].astype(jnp.float32)
            + other_ref[:, columns].astype(jnp.float32)
        )
    for block, value in enumerate(rotate_blocks(mixed, table_ref, stacked_ref)):
        columns = pl.ds(block * DENSE, DENSE)
        start = 0
        for chunk, size in enumerate(sizes):
            piece = value[start : start + size]
            start += size
            out_refs[2 * chunk][:, columns] = piece
            out_refs[2 * chunk + 1][:, columns] = piece.astype(jnp.bfloat16)


def rotate(own, other, me, table, sizes):
    rows, width = own.shape
    shapes = []
    for size in sizes:
        shapes.append(jax.ShapeDtypeStruct((size, width), jnp.float32))
        shapes.append(jax.ShapeDtypeStruct((size, width), jnp.bfloat16))
    return pl.pallas_call(
        functools.partial(rotate_kernel, sizes),
        out_shape=shapes,
        in_specs=[SMEM, ANY, ANY, ANY],
        out_specs=[VMEM] * len(shapes),
        scratch_shapes=[
            pltpu.VMEM((rows * width // DENSE, DENSE), jnp.bfloat16),
            pltpu.VMEM(own.shape, own.dtype),
            pltpu.VMEM(other.shape, other.dtype),
            pltpu.VMEM(table.shape, table.dtype),
            pltpu.SemaphoreType.DMA((3,)),
        ],
        compiler_params=pltpu.CompilerParams(vmem_limit_bytes=20 * 2**20),
        cost_estimate=cost(2 * rows * width * DENSE),
        name="rotate",
    )(me, *[pltpu.with_memory_space_constraint(value, pltpu.HBM) for value in (own, other, table)])


def dequantize_kernel(group_size, packed_ref, scales_ref, weights_ref):
    words = packed_ref.shape[1]
    share = packed_ref.shape[0] // group_size
    for part in range(share):
        group = pl.program_id(0) * share + part
        rows = pl.ds(part * group_size, group_size)
        word = packed_ref[rows, :] ^ np.int32(-2004318072)
        for nibble in range(NIBBLES):
            codes = jnp.right_shift(jnp.left_shift(word, 28 - 4 * nibble), 28)
            scale = scales_ref[pl.ds(group, 1), pl.ds(nibble * words, words)]
            weights_ref[nibble, rows, :] = (codes * scale).astype(jnp.int8)


def dequantize(packed, group_scales):
    width, words = packed.shape
    group_count = group_scales.shape[0]
    group_size = width // group_count
    rows = group_size * (2 - group_count % 2)
    return pl.pallas_call(
        functools.partial(dequantize_kernel, group_size),
        grid=(width // rows,),
        out_shape=pltpu.HBM((NIBBLES, width, words), jnp.int8),
        in_specs=[
            pl.BlockSpec((rows, words), lambda i: (i, 0)),
            pl.BlockSpec(group_scales.shape, lambda i: (0, 0)),
        ],
        out_specs=pl.BlockSpec((NIBBLES, rows, words), lambda i: (0, i, 0)),
        compiler_params=pltpu.CompilerParams(vmem_limit_bytes=12 * 2**20),
        cost_estimate=cost(width * words * 8 * 1024),
        name="dequantize",
    )(
        pltpu.with_memory_space_constraint(packed, pltpu.HBM),
        pltpu.with_memory_space_constraint(group_scales, pltpu.HBM),
    )


def project_kernel(count, unit, rotate_first, me_ref, *refs):
    total = count + rotate_first
    parts, refs = refs[:total], refs[total:]
    weights_ref, keep_ref, send_ref, rotated_ref, buffer, sems = refs[:6]
    staged, staged_sems = refs[6 : 6 + total], refs[6 + total]
    stacked_ref = refs[-1]
    moves = [
        pltpu.make_async_copy(parts[r], staged[r], staged_sems.at[r]) for r in range(total)
    ]
    for move in moves:
        move.start()
    for n in range(NIBBLES):
        pltpu.make_async_copy(weights_ref.at[n], buffer.at[n], sems.at[n]).start()
    for move in moves:
        move.wait()
    parts, table_ref = staged[:count], staged[-1]
    rows, width = parts[0].shape
    words = weights_ref.shape[2]
    blocks = width // DENSE
    me = me_ref[0]
    signs = []
    for r in range(count):
        bits = me & (me ^ r) if rotate_first else jnp.right_shift(me, 1) & (1 - r)
        parity = bits & 1
        for shift in range(1, max(count.bit_length() - 1, 1)):
            parity = parity ^ (jnp.right_shift(bits, shift) & 1)
        signs.append(sign_of(parity))
    mixed = []
    for block in range(blocks):
        columns = pl.ds(block * DENSE, DENSE)
        total = signs[0] * parts[0][:, columns].astype(jnp.float32)
        for r in range(1, count):
            total = total + signs[r] * parts[r][:, columns].astype(jnp.float32)
        mixed.append(total)
    if rotate_first:
        mixed = rotate_blocks(mixed, table_ref, stacked_ref)
    for block in range(blocks):
        rotated_ref[:, pl.ds(block * DENSE, DENSE)] = (mixed[block] * unit).astype(jnp.bfloat16)
    half = rows // 2
    upper = me & 1 == 1

    @pl.loop(0, NIBBLES)
    def _(nibble):
        pltpu.make_async_copy(weights_ref.at[nibble], buffer.at[nibble], sems.at[nibble]).wait()
        product = jnp.dot(
            rotated_ref[...],
            buffer[nibble].astype(jnp.bfloat16),
            preferred_element_type=jnp.float32,
        )
        first, second = product[:half], product[half:]
        columns = pl.ds(pl.multiple_of(nibble * words, words), words)
        keep_ref[:, columns] = jnp.where(upper, second, first)
        send_ref[:, columns] = jnp.where(upper, first, second).astype(jnp.bfloat16)


def project(parts, me, table, weights, unit):
    count = len(parts)
    rows, width = parts[0].shape
    words = weights.shape[2]
    features = NIBBLES * words
    operands = list(parts)
    if table is not None:
        operands.append(pltpu.with_memory_space_constraint(table, pltpu.HBM))
    return pl.pallas_call(
        functools.partial(project_kernel, count, unit, table is not None),
        out_shape=(
            jax.ShapeDtypeStruct((rows // 2, features), jnp.float32),
            jax.ShapeDtypeStruct((rows // 2, features), jnp.bfloat16),
        ),
        in_specs=[SMEM] + [ANY] * len(operands) + [HBM],
        out_specs=(VMEM, VMEM),
        scratch_shapes=[
            pltpu.VMEM((rows, width), jnp.bfloat16),
            pltpu.VMEM(weights.shape, jnp.int8),
            pltpu.SemaphoreType.DMA((NIBBLES,)),
            *[pltpu.VMEM(operand.shape, operand.dtype) for operand in operands],
            pltpu.SemaphoreType.DMA((len(operands),)),
            pltpu.VMEM((rows * width // DENSE, DENSE), jnp.bfloat16),
        ],
        compiler_params=pltpu.CompilerParams(vmem_limit_bytes=28 * 2**20),
        cost_estimate=cost(2 * 128 * width * features),
        name="project",
    )(
        me,
        *operands,
        pltpu.with_memory_space_constraint(weights, pltpu.HBM),
    )


def finish_kernel(sizes, scale, *refs):
    chunks = len(sizes)
    keeps, gots = refs[:chunks], refs[chunks : 2 * chunks]
    residual_ref, new_ref, normed_ref = refs[2 * chunks :]
    start = 0
    for chunk, size in enumerate(sizes):
        rows = pl.ds(start, size)
        start += size
        branch = (keeps[chunk][...] + gots[chunk][...].astype(jnp.float32)) * scale
        fresh = (residual_ref[rows, :].astype(jnp.float32) + branch).astype(jnp.bfloat16)
        new_ref[rows, :] = fresh
        values = fresh.astype(jnp.float32)
        inverse = lax.rsqrt(jnp.mean(values * values, axis=1, keepdims=True) + 1e-05)
        normed_ref[rows, :] = (values * inverse).astype(jnp.bfloat16)


def finish(keeps, gots, residual, scale):
    chunks = len(keeps)
    shape = jax.ShapeDtypeStruct(residual.shape, jnp.bfloat16)
    return pl.pallas_call(
        functools.partial(finish_kernel, [keep.shape[0] for keep in keeps], scale),
        out_shape=(shape, shape),
        in_specs=[VMEM] * (2 * chunks + 1),
        out_specs=(VMEM, VMEM),
        compiler_params=pltpu.CompilerParams(vmem_limit_bytes=12 * 2**20),
        cost_estimate=cost(residual.size * 1024),
        name="finish",
    )(*keeps, *gots, residual)


def local(hidden, signs, packed, group_scales, residual):
    groups = lax.axis_size("tensor")
    bits = groups.bit_length() - 1
    me = lax.axis_index("tensor")
    where = me.reshape(1)
    total_width = hidden.shape[1] * groups
    sizes = chunk_rows(residual.shape[0])
    chunks = len(sizes)
    unit = 1.0 / math.sqrt(total_width)
    table = jnp.asarray(dense_table(), jnp.bfloat16)

    def swap(value, bit):
        return lax.ppermute(value, "tensor", [(i, i ^ (1 << bit)) for i in range(groups)])

    def bit_of(bit):
        return jnp.right_shift(me, bit) & 1

    (first,) = prepare(hidden, signs, groups, [(0, sizes[0])], 1)
    have = {0: first}
    for bit in reversed(range(bits)):
        have.update({r ^ (1 << bit): swap(value, bit) for r, value in list(have.items())})
    stages = [([have[r] for r in range(groups)], table)]
    if chunks > 1:
        places = [(sum(sizes[:chunk]), sizes[chunk]) for chunk in range(1, chunks)]
        sent, own = prepare(hidden, signs, groups, places, 2)
        other = swap(sent, 0)
        pairs = rotate(own, other, where, table, [groups * size for size in sizes[1:]])
        for chunk in range(1, chunks):
            keep, send = pairs[2 * chunk - 2], pairs[2 * chunk - 1]
            for bit in range(1, bits):
                got = swap(send, bit)
                if bit < bits - 1:
                    keep = sign_of(bit_of(bit)) * keep + got.astype(jnp.float32)
                    send = keep.astype(jnp.bfloat16)
            stages.append(([keep, got], None))
    weights = dequantize(packed, group_scales)
    keeps, gots = [], []
    for parts, maybe_table in stages:
        value, send = project(parts, where, maybe_table, weights, unit)
        got = swap(send, 0)
        for bit in range(1, bits):
            value = value + got.astype(jnp.float32)
            half = value.shape[0] // 2
            upper = bit_of(bit) == 1
            send = jnp.where(upper, value[:half], value[half:]).astype(jnp.bfloat16)
            value = jnp.where(upper, value[half:], value[:half])
            got = swap(send, bit)
        keeps.append(value)
        gots.append(got)
    return finish(keeps, gots, residual, 1.0 / (45.0 * math.sqrt(total_width)))


def solution(mesh):
    return jax.shard_map(
        local,
        mesh=mesh,
        in_specs=(
            P("dp", "tensor"),
            P("tensor"),
            P("tensor", None),
            P("tensor", None),
            P(("dp", "tensor"), None),
        ),
        out_specs=(P(("dp", "tensor"), None), P(("dp", "tensor"), None)),
        check_vma=False,
    )
```

```python
import functools
import math

import jax
import jax.numpy as jnp
import numpy as np
from jax import lax
from jax.experimental import pallas as pl
from jax.experimental.pallas import tpu as pltpu
from jax.sharding import PartitionSpec as P


ORDER = 28
DENSE = 896
TILE_ROWS = 16
VMEM = pl.BlockSpec(memory_space=pltpu.VMEM)
SMEM = pl.BlockSpec(memory_space=pltpu.SMEM)
HBM = pl.BlockSpec(memory_space=pltpu.HBM)
BYTES = 4
GRANT = 16


def chunk_rows(token_rows):
    quarter = token_rows // 4
    if quarter % TILE_ROWS:
        return [token_rows]
    return [quarter, 2 * quarter, quarter]


def paley_table():
    offsets = (np.arange(13)[None, :] - np.arange(13)[:, None]) % 13
    residues = np.zeros(13)
    residues[np.arange(1, 13) ** 2 % 13] = 1.0
    quadratic = np.where(offsets == 0, 0.0, np.where(residues[offsets] > 0, 1.0, -1.0))
    conference = np.zeros((14, 14))
    conference[0, 1:] = 1.0
    conference[1:, 0] = 1.0
    conference[1:, 1:] = quadratic
    upper = np.array([[1.0, 1.0], [1.0, -1.0]])
    lower = np.array([[1.0, -1.0], [-1.0, -1.0]])
    return np.kron(conference, upper) + np.kron(np.eye(14), lower)


def sylvester(order):
    table = np.ones((1, 1))
    while table.shape[0] < order:
        table = np.kron(np.array([[1.0, 1.0], [1.0, -1.0]]), table)
    return table


def cost(flops):
    return pl.CostEstimate(flops=flops, bytes_accessed=0, transcendentals=0)


def dense_table():
    return np.kron(sylvester(DENSE // ORDER), paley_table().T)


def bit_reversed(groups):
    bits = groups.bit_length() - 1
    return [sum(((d >> b) & 1) << (bits - 1 - b) for b in range(bits)) for d in range(groups)]


def sign_of(bit):
    return (1 - 2 * bit).astype(jnp.float32)


def prepare_kernel(groups, token_rows, places, hidden_ref, signs_ref, out_ref, staged, sems):
    width = hidden_ref.shape[1]
    copies, at = [], 0
    for start, size in places:
        for owner in bit_reversed(groups):
            copies.append(
                pltpu.make_async_copy(
                    hidden_ref.at[pl.ds(owner * token_rows + start, size), :],
                    staged.at[pl.ds(at, size), :],
                    sems.at[len(copies)],
                )
            )
            copies[-1].start()
            at += size
    flips = (2 * signs_ref[...] - 1).astype(jnp.float32).reshape(1, width)
    at = 0
    for index, copy in enumerate(copies):
        size = places[index // groups][1]
        copy.wait()
        rows = pl.ds(at, size)
        out_ref[rows, :] = (staged[rows, :].astype(jnp.float32) * flips).astype(jnp.bfloat16)
        at += size


def prepare(hidden, signs, groups, places):
    width = hidden.shape[1]
    rows = groups * sum(size for _, size in places)
    count = groups * len(places)
    return pl.pallas_call(
        functools.partial(prepare_kernel, groups, hidden.shape[0] // groups, places),
        out_shape=jax.ShapeDtypeStruct((rows, width), jnp.bfloat16),
        in_specs=[HBM, VMEM],
        out_specs=VMEM,
        scratch_shapes=[
            pltpu.VMEM((rows, width), jnp.bfloat16),
            pltpu.SemaphoreType.DMA((count,)),
        ],
        compiler_params=pltpu.CompilerParams(vmem_limit_bytes=12 * 2**20),
        cost_estimate=cost(rows * width),
        name="prepare",
    )(pltpu.with_memory_space_constraint(hidden, pltpu.HBM), signs)


def rotate_blocks(mixed, table_ref, stacked_ref):
    rows = mixed[0].shape[0]
    blocks = len(mixed)
    span = 1
    while span < blocks:
        for first in range(blocks):
            if not first & span:
                a, b = mixed[first], mixed[first + span]
                mixed[first], mixed[first + span] = a + b, a - b
        span *= 2
    for block in range(blocks):
        stacked_ref[pl.ds(block * rows, rows), :] = mixed[block].astype(jnp.bfloat16)
    turned = jnp.dot(stacked_ref[...], table_ref[...], preferred_element_type=jnp.float32)
    return [turned[block * rows : (block + 1) * rows] for block in range(blocks)]


def rotate_kernel(groups, places, me_ref, hidden_ref, signs_ref, other_ref, table_ref, *refs):
    out_refs, stacked_ref = refs[:-1], refs[-1]
    width = hidden_ref.shape[1]
    token_rows = hidden_ref.shape[0] // groups
    flips = (2 * signs_ref[...] - 1).astype(jnp.float32).reshape(1, width)
    flips = flips * sign_of(me_ref[0] & 1)
    mixed = []
    for block in range(width // DENSE):
        columns = pl.ds(block * DENSE, DENSE)
        own = [
            hidden_ref[pl.ds(owner * token_rows + start, size), columns]
            for start, size in places
            for owner in bit_reversed(groups)
        ]
        own = jnp.concatenate(own, axis=0).astype(jnp.float32)
        turned = own * flips[:, block * DENSE : (block + 1) * DENSE]
        mixed.append(turned + other_ref[:, columns].astype(jnp.float32))
    for block, value in enumerate(rotate_blocks(mixed, table_ref, stacked_ref)):
        columns = pl.ds(block * DENSE, DENSE)
        start = 0
        for chunk, (_, size) in enumerate(places):
            piece = value[start : start + groups * size]
            start += groups * size
            out_refs[2 * chunk][:, columns] = piece
            out_refs[2 * chunk + 1][:, columns] = piece.astype(jnp.bfloat16)


def rotate(hidden, signs, other, me, table, groups, places):
    rows, width = other.shape
    shapes = []
    for _, size in places:
        shapes.append(jax.ShapeDtypeStruct((groups * size, width), jnp.float32))
        shapes.append(jax.ShapeDtypeStruct((groups * size, width), jnp.bfloat16))
    return pl.pallas_call(
        functools.partial(rotate_kernel, groups, places),
        out_shape=shapes,
        in_specs=[SMEM, VMEM, VMEM, VMEM, VMEM],
        out_specs=[VMEM] * len(shapes),
        scratch_shapes=[pltpu.VMEM((rows * width // DENSE, DENSE), jnp.bfloat16)],
        compiler_params=pltpu.CompilerParams(vmem_limit_bytes=20 * 2**20),
        cost_estimate=cost(2 * rows * width * DENSE),
        name="rotate",
    )(me, hidden, signs, other, table)


def dequantize_kernel(packed_ref, bytes_ref):
    word = packed_ref[...] ^ np.int32(-2139062144)
    for place in range(BYTES):
        moved = jnp.right_shift(jnp.left_shift(word, 24 - 8 * place), 24)
        bytes_ref[place, :, :] = moved.astype(jnp.int8)


def dequantize(packed, group_count):
    width, words = packed.shape
    rows = width // group_count * 7 if group_count % 7 == 0 else width // group_count
    return pl.pallas_call(
        dequantize_kernel,
        grid=(width // rows,),
        out_shape=jax.ShapeDtypeStruct((BYTES, width, words), jnp.int8),
        in_specs=[pl.BlockSpec((rows, words), lambda i: (i, 0))],
        out_specs=pl.BlockSpec((BYTES, rows, words), lambda i: (0, i, 0)),
        compiler_params=pltpu.CompilerParams(vmem_limit_bytes=16 * 2**20),
        cost_estimate=cost(width * words * 8 * 512),
        name="dequantize",
    )(pltpu.with_memory_space_constraint(packed, pltpu.HBM))


def project_kernel(count, unit, rotate_first, me_ref, *refs):
    parts, refs = refs[:count], refs[count:]
    if rotate_first:
        table_ref, refs = refs[0], refs[1:]
    scales_ref, bytes_ref, keep_ref, send_ref, rotated_ref, stacked_ref = refs
    rows, width = parts[0].shape
    words = bytes_ref.shape[2]
    group_count = scales_ref.shape[0]
    group_size = width // group_count
    blocks = width // DENSE
    me = me_ref[0]
    signs = []
    for r in range(count):
        bits = me & (me ^ r) if rotate_first else jnp.right_shift(me, 1) & (1 - r)
        parity = bits & 1
        for shift in range(1, max(count.bit_length() - 1, 1)):
            parity = parity ^ (jnp.right_shift(bits, shift) & 1)
        signs.append(sign_of(parity))
    mixed = []
    for block in range(blocks):
        columns = pl.ds(block * DENSE, DENSE)
        total = signs[0] * parts[0][:, columns].astype(jnp.float32)
        for r in range(1, count):
            total = total + signs[r] * parts[r][:, columns].astype(jnp.float32)
        mixed.append(total)
    if rotate_first:
        mixed = rotate_blocks(mixed, table_ref, stacked_ref)
    for block in range(blocks):
        rotated_ref[:, pl.ds(block * DENSE, DENSE)] = (mixed[block] * unit).astype(jnp.bfloat16)
    half = rows // 2
    upper = me & 1 == 1

    @pl.loop(0, BYTES)
    def _(place):
        spans = [
            pl.ds(pl.multiple_of((2 * place + side) * words, words), words) for side in range(2)
        ]
        sides = [[], []]
        for group in range(group_count):
            both = bytes_ref[place, group * group_size : (group + 1) * group_size, :]
            high = (both & jnp.int8(-16)).astype(jnp.bfloat16)
            low = both.astype(jnp.bfloat16) - high - jnp.bfloat16(8)
            sides[0].append(low * scales_ref[group : group + 1, spans[0]])
            sides[1].append(high * scales_ref[group : group + 1, spans[1]])
        for columns, weights in zip(spans, sides):
            product = jnp.dot(
                rotated_ref[...],
                jnp.concatenate(weights, axis=0),
                preferred_element_type=jnp.float32,
            )
            first, second = product[:half], product[half:]
            keep_ref[:, columns] = jnp.where(upper, second, first)
            send_ref[:, columns] = jnp.where(upper, first, second).astype(jnp.bfloat16)


def project(parts, me, table, scales, weights, unit):
    count = len(parts)
    rows, width = parts[0].shape
    features = scales.shape[1]
    tables = [] if table is None else [table]
    return pl.pallas_call(
        functools.partial(project_kernel, count, unit, table is not None),
        out_shape=(
            jax.ShapeDtypeStruct((rows // 2, features), jnp.float32),
            jax.ShapeDtypeStruct((rows // 2, features), jnp.bfloat16),
        ),
        in_specs=[SMEM] + [VMEM] * (count + len(tables) + 2),
        out_specs=(VMEM, VMEM),
        scratch_shapes=[
            pltpu.VMEM((rows, width), jnp.bfloat16),
            pltpu.VMEM((rows * width // DENSE, DENSE), jnp.bfloat16),
        ],
        compiler_params=pltpu.CompilerParams(vmem_limit_bytes=GRANT * 2**20),
        cost_estimate=cost(2 * 128 * width * features),
        name="project",
    )(me, *parts, *tables, scales, weights)


def finish_kernel(sizes, scale, *refs):
    chunks = len(sizes)
    keeps, gots = refs[:chunks], refs[chunks : 2 * chunks]
    residual_ref, new_ref, normed_ref = refs[2 * chunks :]
    start = 0
    for chunk, size in enumerate(sizes):
        rows = pl.ds(start, size)
        start += size
        branch = (keeps[chunk][...] + gots[chunk][...].astype(jnp.float32)) * scale
        fresh = (residual_ref[rows, :].astype(jnp.float32) + branch).astype(jnp.bfloat16)
        new_ref[rows, :] = fresh
        values = fresh.astype(jnp.float32)
        inverse = lax.rsqrt(jnp.mean(values * values, axis=1, keepdims=True) + 1e-05)
        normed_ref[rows, :] = (values * inverse).astype(jnp.bfloat16)


def finish(keeps, gots, residual, scale):
    chunks = len(keeps)
    shape = jax.ShapeDtypeStruct(residual.shape, jnp.bfloat16)
    return pl.pallas_call(
        functools.partial(finish_kernel, [keep.shape[0] for keep in keeps], scale),
        out_shape=(shape, shape),
        in_specs=[VMEM] * (2 * chunks + 1),
        out_specs=(VMEM, VMEM),
        compiler_params=pltpu.CompilerParams(vmem_limit_bytes=12 * 2**20),
        cost_estimate=cost(residual.size * 1024),
        name="finish",
    )(*keeps, *gots, residual)


def local(hidden, signs, packed, group_scales, residual):
    groups = lax.axis_size("tensor")
    bits = groups.bit_length() - 1
    me = lax.axis_index("tensor")
    where = me.reshape(1)
    total_width = hidden.shape[1] * groups
    sizes = chunk_rows(residual.shape[0])
    chunks = len(sizes)
    unit = 1.0 / math.sqrt(total_width)
    table = jnp.asarray(dense_table(), jnp.bfloat16)

    def swap(value, bit):
        return lax.ppermute(value, "tensor", [(i, i ^ (1 << bit)) for i in range(groups)])

    def bit_of(bit):
        return jnp.right_shift(me, bit) & 1

    first = prepare(hidden, signs, groups, [(0, sizes[0])])
    have = {0: first}
    for bit in reversed(range(bits)):
        have.update({r ^ (1 << bit): swap(value, bit) for r, value in list(have.items())})
    stages = [([have[r] for r in range(groups)], table)]
    if chunks > 1:
        places = [(sum(sizes[:chunk]), sizes[chunk]) for chunk in range(1, chunks)]
        sent = prepare(hidden, signs, groups, places)
        other = swap(sent, 0)
        pairs = rotate(hidden, signs, other, where, table, groups, places)
        for chunk in range(1, chunks):
            keep, send = pairs[2 * chunk - 2], pairs[2 * chunk - 1]
            for bit in range(1, bits):
                got = swap(send, bit)
                if bit < bits - 1:
                    keep = sign_of(bit_of(bit)) * keep + got.astype(jnp.float32)
                    send = keep.astype(jnp.bfloat16)
            stages.append(([keep, got], None))
    weights = dequantize(packed, group_scales.shape[0])
    words = packed.shape[1]
    side = jnp.arange(group_scales.shape[1]) // words % 2
    scales = group_scales.astype(jnp.float32) * jnp.where(side == 1, 0.0625, 1.0)[None, :]
    scales = scales.astype(jnp.bfloat16)
    keeps, gots = [], []
    for parts, maybe_table in stages:
        value, send = project(parts, where, maybe_table, scales, weights, unit)
        got = swap(send, 0)
        for bit in range(1, bits):
            value = value + got.astype(jnp.float32)
            half = value.shape[0] // 2
            upper = bit_of(bit) == 1
            send = jnp.where(upper, value[:half], value[half:]).astype(jnp.bfloat16)
            value = jnp.where(upper, value[half:], value[:half])
            got = swap(send, bit)
        keeps.append(value)
        gots.append(got)
    return finish(keeps, gots, residual, 1.0 / (45.0 * math.sqrt(total_width)))


def solution(mesh):
    return jax.shard_map(
        local,
        mesh=mesh,
        in_specs=(
            P("dp", "tensor"),
            P("tensor"),
            P("tensor", None),
            P("tensor", None),
            P(("dp", "tensor"), None),
        ),
        out_specs=(P(("dp", "tensor"), None), P(("dp", "tensor"), None)),
        check_vma=False,
    )
```

```python
import functools
import math

import jax
import jax.numpy as jnp
import numpy as np
from jax import lax
from jax.experimental import pallas as pl
from jax.experimental.pallas import tpu as pltpu
from jax.sharding import PartitionSpec as P


ORDER = 28
DENSE = 896
TILE_ROWS = 16
VMEM = pl.BlockSpec(memory_space=pltpu.VMEM)
SMEM = pl.BlockSpec(memory_space=pltpu.SMEM)
HBM = pl.BlockSpec(memory_space=pltpu.HBM)
BYTES = 4
GRANT = 16


def chunk_rows(token_rows):
    quarter = token_rows // 4
    if quarter % TILE_ROWS:
        return [token_rows]
    return [quarter, 2 * quarter, quarter]


def paley_table():
    offsets = (np.arange(13)[None, :] - np.arange(13)[:, None]) % 13
    residues = np.zeros(13)
    residues[np.arange(1, 13) ** 2 % 13] = 1.0
    quadratic = np.where(offsets == 0, 0.0, np.where(residues[offsets] > 0, 1.0, -1.0))
    conference = np.zeros((14, 14))
    conference[0, 1:] = 1.0
    conference[1:, 0] = 1.0
    conference[1:, 1:] = quadratic
    upper = np.array([[1.0, 1.0], [1.0, -1.0]])
    lower = np.array([[1.0, -1.0], [-1.0, -1.0]])
    return np.kron(conference, upper) + np.kron(np.eye(14), lower)


def sylvester(order):
    table = np.ones((1, 1))
    while table.shape[0] < order:
        table = np.kron(np.array([[1.0, 1.0], [1.0, -1.0]]), table)
    return table


def cost(flops):
    return pl.CostEstimate(flops=flops, bytes_accessed=0, transcendentals=0)


def dense_table():
    return np.kron(sylvester(DENSE // ORDER), paley_table().T)


def bit_reversed(groups):
    bits = groups.bit_length() - 1
    return [sum(((d >> b) & 1) << (bits - 1 - b) for b in range(bits)) for d in range(groups)]


def sign_of(bit):
    return (1 - 2 * bit).astype(jnp.float32)


def prepare_kernel(groups, token_rows, places, hidden_ref, signs_ref, *refs):
    out_refs, (staged, flips, sems, flips_sem) = refs[:-4], refs[-4:]
    width = hidden_ref.shape[1]
    flips_copy = pltpu.make_async_copy(signs_ref, flips, flips_sem)
    flips_copy.start()
    copies, at = [], 0
    for start, size in places:
        for owner in bit_reversed(groups):
            copies.append(
                pltpu.make_async_copy(
                    hidden_ref.at[pl.ds(owner * token_rows + start, size), :],
                    staged.at[pl.ds(at, size), :],
                    sems.at[len(copies)],
                )
            )
            copies[-1].start()
            at += size
    flips_copy.wait()
    flip = (2 * flips[...] - 1).astype(jnp.float32).reshape(1, width)
    first_rows = groups * places[0][1]
    at = 0
    for index, copy in enumerate(copies):
        size = places[index // groups][1]
        copy.wait()
        value = (staged[pl.ds(at, size), :].astype(jnp.float32) * flip).astype(jnp.bfloat16)
        if index < groups:
            out_refs[0][pl.ds(at, size), :] = value
        else:
            out_refs[1][pl.ds(at - first_rows, size), :] = value
        at += size


def prepare(hidden, signs, groups, places):
    rows, width = hidden.shape
    first_rows = groups * places[0][1]
    shapes = [pltpu.VMEM((first_rows, width), jnp.bfloat16)]
    if len(places) > 1:
        shapes.append(pltpu.VMEM((rows - first_rows, width), jnp.bfloat16))
    return pl.pallas_call(
        functools.partial(prepare_kernel, groups, rows // groups, places),
        out_shape=shapes,
        in_specs=[HBM, HBM],
        out_specs=[VMEM] * len(shapes),
        scratch_shapes=[
            pltpu.VMEM((rows, width), jnp.bfloat16),
            pltpu.VMEM((width,), jnp.int32),
            pltpu.SemaphoreType.DMA((groups * len(places),)),
            pltpu.SemaphoreType.DMA,
        ],
        compiler_params=pltpu.CompilerParams(vmem_limit_bytes=8 * 2**20),
        cost_estimate=cost(rows * width),
        name="prepare",
    )(*[pltpu.with_memory_space_constraint(value, pltpu.HBM) for value in (hidden, signs)])


def rotate_blocks(mixed, table_ref, stacked_ref):
    rows = mixed[0].shape[0]
    blocks = len(mixed)
    span = 1
    while span < blocks:
        for first in range(blocks):
            if not first & span:
                a, b = mixed[first], mixed[first + span]
                mixed[first], mixed[first + span] = a + b, a - b
        span *= 2
    for block in range(blocks):
        stacked_ref[pl.ds(block * rows, rows), :] = mixed[block].astype(jnp.bfloat16)
    turned = jnp.dot(stacked_ref[...], table_ref[...], preferred_element_type=jnp.float32)
    return [turned[block * rows : (block + 1) * rows] for block in range(blocks)]


def rotate_kernel(groups, places, me_ref, hidden_ref, signs_ref, other_ref, table_ref, *refs):
    out_refs, stacked_ref = refs[:-1], refs[-1]
    width = hidden_ref.shape[1]
    token_rows = hidden_ref.shape[0] // groups
    flips = (2 * signs_ref[...] - 1).astype(jnp.float32).reshape(1, width)
    flips = flips * sign_of(me_ref[0] & 1)
    mixed = []
    for block in range(width // DENSE):
        columns = pl.ds(block * DENSE, DENSE)
        own = [
            hidden_ref[pl.ds(owner * token_rows + start, size), columns]
            for start, size in places
            for owner in bit_reversed(groups)
        ]
        own = jnp.concatenate(own, axis=0).astype(jnp.float32)
        turned = own * flips[:, block * DENSE : (block + 1) * DENSE]
        mixed.append(turned + other_ref[:, columns].astype(jnp.float32))
    for block, value in enumerate(rotate_blocks(mixed, table_ref, stacked_ref)):
        columns = pl.ds(block * DENSE, DENSE)
        start = 0
        for chunk, (_, size) in enumerate(places):
            piece = value[start : start + groups * size]
            start += groups * size
            out_refs[2 * chunk][:, columns] = piece
            out_refs[2 * chunk + 1][:, columns] = piece.astype(jnp.bfloat16)


def rotate(hidden, signs, other, me, table, groups, places):
    rows, width = other.shape
    shapes = []
    for _, size in places:
        shapes.append(jax.ShapeDtypeStruct((groups * size, width), jnp.float32))
        shapes.append(jax.ShapeDtypeStruct((groups * size, width), jnp.bfloat16))
    return pl.pallas_call(
        functools.partial(rotate_kernel, groups, places),
        out_shape=shapes,
        in_specs=[SMEM, VMEM, VMEM, VMEM, VMEM],
        out_specs=[VMEM] * len(shapes),
        scratch_shapes=[pltpu.VMEM((rows * width // DENSE, DENSE), jnp.bfloat16)],
        compiler_params=pltpu.CompilerParams(vmem_limit_bytes=20 * 2**20),
        cost_estimate=cost(2 * rows * width * DENSE),
        name="rotate",
    )(me, hidden, signs, other, table)


def dequantize_kernel(packed_ref, bytes_ref):
    word = packed_ref[...] ^ np.int32(-2139062144)
    for place in range(BYTES):
        moved = jnp.right_shift(jnp.left_shift(word, 24 - 8 * place), 24)
        bytes_ref[place, :, :] = moved.astype(jnp.int8)


def dequantize(packed, group_count):
    width, words = packed.shape
    rows = width // group_count * 7 if group_count % 7 == 0 else width // group_count
    return pl.pallas_call(
        dequantize_kernel,
        grid=(width // rows,),
        out_shape=jax.ShapeDtypeStruct((BYTES, width, words), jnp.int8),
        in_specs=[pl.BlockSpec((rows, words), lambda i: (i, 0))],
        out_specs=pl.BlockSpec((BYTES, rows, words), lambda i: (0, i, 0)),
        compiler_params=pltpu.CompilerParams(vmem_limit_bytes=16 * 2**20),
        cost_estimate=cost(width * words * 8 * 512),
        name="dequantize",
    )(pltpu.with_memory_space_constraint(packed, pltpu.HBM))


def project_kernel(count, unit, rotate_first, me_ref, *refs):
    parts, refs = refs[:count], refs[count:]
    if rotate_first:
        table_ref, refs = refs[0], refs[1:]
    scales_ref, bytes_ref, keep_ref, send_ref, rotated_ref, stacked_ref = refs
    rows, width = parts[0].shape
    words = bytes_ref.shape[2]
    group_count = scales_ref.shape[0]
    group_size = width // group_count
    blocks = width // DENSE
    me = me_ref[0]
    signs = []
    for r in range(count):
        bits = me & (me ^ r) if rotate_first else jnp.right_shift(me, 1) & (1 - r)
        parity = bits & 1
        for shift in range(1, max(count.bit_length() - 1, 1)):
            parity = parity ^ (jnp.right_shift(bits, shift) & 1)
        signs.append(sign_of(parity))
    mixed = []
    for block in range(blocks):
        columns = pl.ds(block * DENSE, DENSE)
        total = signs[0] * parts[0][:, columns].astype(jnp.float32)
        for r in range(1, count):
            total = total + signs[r] * parts[r][:, columns].astype(jnp.float32)
        mixed.append(total)
    if rotate_first:
        mixed = rotate_blocks(mixed, table_ref, stacked_ref)
    for block in range(blocks):
        rotated_ref[:, pl.ds(block * DENSE, DENSE)] = (mixed[block] * unit).astype(jnp.bfloat16)
    half = rows // 2
    upper = me & 1 == 1

    @pl.loop(0, BYTES)
    def _(place):
        spans = [
            pl.ds(pl.multiple_of((2 * place + side) * words, words), words) for side in range(2)
        ]
        sides = [[], []]
        for group in range(group_count):
            both = bytes_ref[place, group * group_size : (group + 1) * group_size, :]
            high = (both & jnp.int8(-16)).astype(jnp.bfloat16)
            low = both.astype(jnp.bfloat16) - high - jnp.bfloat16(8)
            sides[0].append(low * scales_ref[group : group + 1, spans[0]])
            sides[1].append(high * scales_ref[group : group + 1, spans[1]])
        for columns, weights in zip(spans, sides):
            product = jnp.dot(
                rotated_ref[...],
                jnp.concatenate(weights, axis=0),
                preferred_element_type=jnp.float32,
            )
            first, second = product[:half], product[half:]
            keep_ref[:, columns] = jnp.where(upper, second, first)
            send_ref[:, columns] = jnp.where(upper, first, second).astype(jnp.bfloat16)


def project(parts, me, table, scales, weights, unit):
    count = len(parts)
    rows, width = parts[0].shape
    features = scales.shape[1]
    tables = [] if table is None else [table]
    return pl.pallas_call(
        functools.partial(project_kernel, count, unit, table is not None),
        out_shape=(
            jax.ShapeDtypeStruct((rows // 2, features), jnp.float32),
            jax.ShapeDtypeStruct((rows // 2, features), jnp.bfloat16),
        ),
        in_specs=[SMEM] + [VMEM] * (count + len(tables) + 2),
        out_specs=(VMEM, VMEM),
        scratch_shapes=[
            pltpu.VMEM((rows, width), jnp.bfloat16),
            pltpu.VMEM((rows * width // DENSE, DENSE), jnp.bfloat16),
        ],
        compiler_params=pltpu.CompilerParams(vmem_limit_bytes=GRANT * 2**20),
        cost_estimate=cost(2 * 128 * width * features),
        name="project",
    )(me, *parts, *tables, scales, weights)


def finish_kernel(sizes, scale, *refs):
    chunks = len(sizes)
    keeps, gots = refs[:chunks], refs[chunks : 2 * chunks]
    residual_ref, new_ref, normed_ref = refs[2 * chunks :]
    start = 0
    for chunk, size in enumerate(sizes):
        rows = pl.ds(start, size)
        start += size
        branch = (keeps[chunk][...] + gots[chunk][...].astype(jnp.float32)) * scale
        fresh = (residual_ref[rows, :].astype(jnp.float32) + branch).astype(jnp.bfloat16)
        new_ref[rows, :] = fresh
        values = fresh.astype(jnp.float32)
        inverse = lax.rsqrt(jnp.mean(values * values, axis=1, keepdims=True) + 1e-05)
        normed_ref[rows, :] = (values * inverse).astype(jnp.bfloat16)


def finish(keeps, gots, residual, scale):
    chunks = len(keeps)
    shape = jax.ShapeDtypeStruct(residual.shape, jnp.bfloat16)
    return pl.pallas_call(
        functools.partial(finish_kernel, [keep.shape[0] for keep in keeps], scale),
        out_shape=(shape, shape),
        in_specs=[VMEM] * (2 * chunks + 1),
        out_specs=(VMEM, VMEM),
        compiler_params=pltpu.CompilerParams(vmem_limit_bytes=12 * 2**20),
        cost_estimate=cost(residual.size * 1024),
        name="finish",
    )(*keeps, *gots, residual)


def local(hidden, signs, packed, group_scales, residual):
    groups = lax.axis_size("tensor")
    bits = groups.bit_length() - 1
    me = lax.axis_index("tensor")
    where = me.reshape(1)
    total_width = hidden.shape[1] * groups
    sizes = chunk_rows(residual.shape[0])
    chunks = len(sizes)
    unit = 1.0 / math.sqrt(total_width)
    table = jnp.asarray(dense_table(), jnp.bfloat16)

    def swap(value, bit):
        return lax.ppermute(value, "tensor", [(i, i ^ (1 << bit)) for i in range(groups)])

    def bit_of(bit):
        return jnp.right_shift(me, bit) & 1

    places = [(sum(sizes[:chunk]), sizes[chunk]) for chunk in range(chunks)]
    first, *sent = prepare(hidden, signs, groups, places)
    have = {0: first}
    for bit in reversed(range(bits)):
        have.update({r ^ (1 << bit): swap(value, bit) for r, value in list(have.items())})
    stages = [([have[r] for r in range(groups)], table)]
    if chunks > 1:
        other = swap(sent[0], 0)
        pairs = rotate(hidden, signs, other, where, table, groups, places[1:])
        for chunk in range(1, chunks):
            keep, send = pairs[2 * chunk - 2], pairs[2 * chunk - 1]
            for bit in range(1, bits):
                got = swap(send, bit)
                if bit < bits - 1:
                    keep = sign_of(bit_of(bit)) * keep + got.astype(jnp.float32)
                    send = keep.astype(jnp.bfloat16)
            stages.append(([keep, got], None))
    weights = dequantize(packed, group_scales.shape[0])
    words = packed.shape[1]
    side = jnp.arange(group_scales.shape[1]) // words % 2
    scales = group_scales.astype(jnp.float32) * jnp.where(side == 1, 0.0625, 1.0)[None, :]
    scales = scales.astype(jnp.bfloat16)
    keeps, gots = [], []
    for parts, maybe_table in stages:
        value, send = project(parts, where, maybe_table, scales, weights, unit)
        got = swap(send, 0)
        for bit in range(1, bits):
            value = value + got.astype(jnp.float32)
            half = value.shape[0] // 2
            upper = bit_of(bit) == 1
            send = jnp.where(upper, value[:half], value[half:]).astype(jnp.bfloat16)
            value = jnp.where(upper, value[half:], value[:half])
            got = swap(send, bit)
        keeps.append(value)
        gots.append(got)
    return finish(keeps, gots, residual, 1.0 / (45.0 * math.sqrt(total_width)))


def solution(mesh):
    return jax.shard_map(
        local,
        mesh=mesh,
        in_specs=(
            P("dp", "tensor"),
            P("tensor"),
            P("tensor", None),
            P("tensor", None),
            P(("dp", "tensor"), None),
        ),
        out_specs=(P(("dp", "tensor"), None), P(("dp", "tensor"), None)),
        check_vma=False,
    )
```

```python
import functools
import math

import jax
import jax.numpy as jnp
import numpy as np
from jax import lax
from jax.experimental import pallas as pl
from jax.experimental.pallas import tpu as pltpu
from jax.sharding import PartitionSpec as P


ORDER = 28
DENSE = 896
TILE_ROWS = 16
VMEM = pl.BlockSpec(memory_space=pltpu.VMEM)
SMEM = pl.BlockSpec(memory_space=pltpu.SMEM)
HBM = pl.BlockSpec(memory_space=pltpu.HBM)
BYTES = 4
GRANT = 16


def chunk_rows(token_rows):
    quarter = token_rows // 4
    if quarter % TILE_ROWS:
        return [token_rows]
    return [quarter, 2 * quarter, quarter]


def paley_table():
    offsets = (np.arange(13)[None, :] - np.arange(13)[:, None]) % 13
    residues = np.zeros(13)
    residues[np.arange(1, 13) ** 2 % 13] = 1.0
    quadratic = np.where(offsets == 0, 0.0, np.where(residues[offsets] > 0, 1.0, -1.0))
    conference = np.zeros((14, 14))
    conference[0, 1:] = 1.0
    conference[1:, 0] = 1.0
    conference[1:, 1:] = quadratic
    upper = np.array([[1.0, 1.0], [1.0, -1.0]])
    lower = np.array([[1.0, -1.0], [-1.0, -1.0]])
    return np.kron(conference, upper) + np.kron(np.eye(14), lower)


def sylvester(order):
    table = np.ones((1, 1))
    while table.shape[0] < order:
        table = np.kron(np.array([[1.0, 1.0], [1.0, -1.0]]), table)
    return table


def cost(flops):
    return pl.CostEstimate(flops=flops, bytes_accessed=0, transcendentals=0)


def dense_table():
    return np.kron(sylvester(DENSE // ORDER), paley_table().T)


def bit_reversed(groups):
    bits = groups.bit_length() - 1
    return [sum(((d >> b) & 1) << (bits - 1 - b) for b in range(bits)) for d in range(groups)]


def sign_of(bit):
    return (1 - 2 * bit).astype(jnp.float32)


def flips_of(signs):
    return (2 * signs - 1).astype(jnp.float32).reshape(1, signs.shape[0])


def open_kernel(groups, token_rows, size, hidden_ref, signs_ref, out_ref, staged, flips, sems):
    copies = [pltpu.make_async_copy(signs_ref, flips, sems.at[groups])]
    for place, owner in enumerate(bit_reversed(groups)):
        copies.append(
            pltpu.make_async_copy(
                hidden_ref.at[pl.ds(owner * token_rows, size), :],
                staged.at[pl.ds(place * size, size), :],
                sems.at[place],
            )
        )
    for copy in copies:
        copy.start()
    for copy in copies:
        copy.wait()
    out_ref[...] = (staged[...].astype(jnp.float32) * flips_of(flips[...])).astype(jnp.bfloat16)


def open_exchange(hidden, signs, groups, size):
    rows, width = groups * size, hidden.shape[1]
    return pl.pallas_call(
        functools.partial(open_kernel, groups, hidden.shape[0] // groups, size),
        out_shape=jax.ShapeDtypeStruct((rows, width), jnp.bfloat16),
        in_specs=[HBM, HBM],
        out_specs=VMEM,
        scratch_shapes=[
            pltpu.VMEM((rows, width), jnp.bfloat16),
            pltpu.VMEM((width,), jnp.int32),
            pltpu.SemaphoreType.DMA((groups + 1,)),
        ],
        compiler_params=pltpu.CompilerParams(vmem_limit_bytes=8 * 2**20),
        cost_estimate=cost(rows * width),
        name="open_exchange",
    )(*[pltpu.with_memory_space_constraint(value, pltpu.HBM) for value in (hidden, signs)])


def prepare_kernel(groups, places, hidden_ref, signs_ref, first_ref, *rest_refs):
    token_rows = hidden_ref.shape[0] // groups
    flips = flips_of(signs_ref[...])
    at, out_ref = 0, first_ref
    for chunk, (start, size) in enumerate(places):
        if chunk == 1:
            at, out_ref = 0, rest_refs[0]
        for owner in bit_reversed(groups):
            rows = hidden_ref[pl.ds(owner * token_rows + start, size), :]
            out_ref[pl.ds(at, size), :] = (rows.astype(jnp.float32) * flips).astype(jnp.bfloat16)
            at += size


def prepare(hidden, signs, groups, places):
    rows, width = hidden.shape
    first_rows = groups * places[0][1]
    shapes = [pltpu.HBM((first_rows, width), jnp.bfloat16)]
    if len(places) > 1:
        shapes.append(jax.ShapeDtypeStruct((rows - first_rows, width), jnp.bfloat16))
    return pl.pallas_call(
        functools.partial(prepare_kernel, groups, places),
        out_shape=shapes,
        in_specs=[VMEM, VMEM],
        out_specs=[VMEM] * len(shapes),
        compiler_params=pltpu.CompilerParams(vmem_limit_bytes=8 * 2**20),
        cost_estimate=cost(rows * width),
        name="prepare",
    )(hidden, signs)


def rotate_blocks(mixed, table_ref, stacked_ref):
    rows = mixed[0].shape[0]
    blocks = len(mixed)
    span = 1
    while span < blocks:
        for first in range(blocks):
            if not first & span:
                a, b = mixed[first], mixed[first + span]
                mixed[first], mixed[first + span] = a + b, a - b
        span *= 2
    for block in range(blocks):
        stacked_ref[pl.ds(block * rows, rows), :] = mixed[block].astype(jnp.bfloat16)
    turned = jnp.dot(stacked_ref[...], table_ref[...], preferred_element_type=jnp.float32)
    return [turned[block * rows : (block + 1) * rows] for block in range(blocks)]


def rotate_kernel(groups, places, me_ref, hidden_ref, signs_ref, other_ref, table_ref, *refs):
    out_refs, stacked_ref = refs[:-1], refs[-1]
    width = hidden_ref.shape[1]
    token_rows = hidden_ref.shape[0] // groups
    flips = (2 * signs_ref[...] - 1).astype(jnp.float32).reshape(1, width)
    flips = flips * sign_of(me_ref[0] & 1)
    mixed = []
    for block in range(width // DENSE):
        columns = pl.ds(block * DENSE, DENSE)
        own = [
            hidden_ref[pl.ds(owner * token_rows + start, size), columns]
            for start, size in places
            for owner in bit_reversed(groups)
        ]
        own = jnp.concatenate(own, axis=0).astype(jnp.float32)
        turned = own * flips[:, block * DENSE : (block + 1) * DENSE]
        mixed.append(turned + other_ref[:, columns].astype(jnp.float32))
    for block, value in enumerate(rotate_blocks(mixed, table_ref, stacked_ref)):
        columns = pl.ds(block * DENSE, DENSE)
        start = 0
        for chunk, (_, size) in enumerate(places):
            piece = value[start : start + groups * size]
            start += groups * size
            out_refs[2 * chunk][:, columns] = piece
            out_refs[2 * chunk + 1][:, columns] = piece.astype(jnp.bfloat16)


def rotate(hidden, signs, other, me, table, groups, places):
    rows, width = other.shape
    shapes = []
    for _, size in places:
        shapes.append(jax.ShapeDtypeStruct((groups * size, width), jnp.float32))
        shapes.append(jax.ShapeDtypeStruct((groups * size, width), jnp.bfloat16))
    return pl.pallas_call(
        functools.partial(rotate_kernel, groups, places),
        out_shape=shapes,
        in_specs=[SMEM, VMEM, VMEM, VMEM, VMEM],
        out_specs=[VMEM] * len(shapes),
        scratch_shapes=[pltpu.VMEM((rows * width // DENSE, DENSE), jnp.bfloat16)],
        compiler_params=pltpu.CompilerParams(vmem_limit_bytes=20 * 2**20),
        cost_estimate=cost(2 * rows * width * DENSE),
        name="rotate",
    )(me, hidden, signs, other, table)


def dequantize_kernel(packed_ref, bytes_ref):
    word = packed_ref[...] ^ np.int32(-2139062144)
    for place in range(BYTES):
        moved = jnp.right_shift(jnp.left_shift(word, 24 - 8 * place), 24)
        bytes_ref[place, :, :] = moved.astype(jnp.int8)


def dequantize(packed, group_count):
    width, words = packed.shape
    rows = width // group_count * 7 if group_count % 7 == 0 else width // group_count
    return pl.pallas_call(
        dequantize_kernel,
        grid=(width // rows,),
        out_shape=jax.ShapeDtypeStruct((BYTES, width, words), jnp.int8),
        in_specs=[pl.BlockSpec((rows, words), lambda i: (i, 0))],
        out_specs=pl.BlockSpec((BYTES, rows, words), lambda i: (0, i, 0)),
        compiler_params=pltpu.CompilerParams(vmem_limit_bytes=16 * 2**20),
        cost_estimate=cost(width * words * 8 * 512),
        name="dequantize",
    )(pltpu.with_memory_space_constraint(packed, pltpu.HBM))


def project_kernel(count, unit, rotate_first, me_ref, *refs):
    parts, refs = refs[:count], refs[count:]
    if rotate_first:
        table_ref, refs = refs[0], refs[1:]
    scales_ref, bytes_ref, keep_ref, send_ref, rotated_ref, stacked_ref = refs
    rows, width = parts[0].shape
    words = bytes_ref.shape[2]
    group_count = scales_ref.shape[0]
    group_size = width // group_count
    blocks = width // DENSE
    me = me_ref[0]
    signs = []
    for r in range(count):
        bits = me & (me ^ r) if rotate_first else jnp.right_shift(me, 1) & (1 - r)
        parity = bits & 1
        for shift in range(1, max(count.bit_length() - 1, 1)):
            parity = parity ^ (jnp.right_shift(bits, shift) & 1)
        signs.append(sign_of(parity))
    mixed = []
    for block in range(blocks):
        columns = pl.ds(block * DENSE, DENSE)
        total = signs[0] * parts[0][:, columns].astype(jnp.float32)
        for r in range(1, count):
            total = total + signs[r] * parts[r][:, columns].astype(jnp.float32)
        mixed.append(total)
    if rotate_first:
        mixed = rotate_blocks(mixed, table_ref, stacked_ref)
    for block in range(blocks):
        rotated_ref[:, pl.ds(block * DENSE, DENSE)] = (mixed[block] * unit).astype(jnp.bfloat16)
    half = rows // 2
    upper = me & 1 == 1

    @pl.loop(0, BYTES)
    def _(place):
        spans = [
            pl.ds(pl.multiple_of((2 * place + side) * words, words), words) for side in range(2)
        ]
        sides = [[], []]
        for group in range(group_count):
            both = bytes_ref[place, group * group_size : (group + 1) * group_size, :]
            high = (both & jnp.int8(-16)).astype(jnp.bfloat16)
            low = both.astype(jnp.bfloat16) - high - jnp.bfloat16(8)
            sides[0].append(low * scales_ref[group : group + 1, spans[0]])
            sides[1].append(high * scales_ref[group : group + 1, spans[1]])
        for columns, weights in zip(spans, sides):
            product = jnp.dot(
                rotated_ref[...],
                jnp.concatenate(weights, axis=0),
                preferred_element_type=jnp.float32,
            )
            first, second = product[:half], product[half:]
            keep_ref[:, columns] = jnp.where(upper, second, first)
            send_ref[:, columns] = jnp.where(upper, first, second).astype(jnp.bfloat16)


def project(parts, me, table, scales, weights, unit):
    count = len(parts)
    rows, width = parts[0].shape
    features = scales.shape[1]
    tables = [] if table is None else [table]
    return pl.pallas_call(
        functools.partial(project_kernel, count, unit, table is not None),
        out_shape=(
            jax.ShapeDtypeStruct((rows // 2, features), jnp.float32),
            jax.ShapeDtypeStruct((rows // 2, features), jnp.bfloat16),
        ),
        in_specs=[SMEM] + [VMEM] * (count + len(tables) + 2),
        out_specs=(VMEM, VMEM),
        scratch_shapes=[
            pltpu.VMEM((rows, width), jnp.bfloat16),
            pltpu.VMEM((rows * width // DENSE, DENSE), jnp.bfloat16),
        ],
        compiler_params=pltpu.CompilerParams(vmem_limit_bytes=GRANT * 2**20),
        cost_estimate=cost(2 * 128 * width * features),
        name="project",
    )(me, *parts, *tables, scales, weights)


def fold_kernel(bit, me_ref, keep_ref, got_ref, value_ref, send_ref):
    half = value_ref.shape[0]
    upper = jnp.right_shift(me_ref[0], bit) & 1 == 1
    first = keep_ref[:half, :] + got_ref[:half, :].astype(jnp.float32)
    second = keep_ref[half:, :] + got_ref[half:, :].astype(jnp.float32)
    value_ref[...] = jnp.where(upper, second, first)
    send_ref[...] = jnp.where(upper, first, second).astype(jnp.bfloat16)


def fold(keep, got, me, bit):
    rows, features = keep.shape
    return pl.pallas_call(
        functools.partial(fold_kernel, bit),
        out_shape=(
            jax.ShapeDtypeStruct((rows // 2, features), jnp.float32),
            jax.ShapeDtypeStruct((rows // 2, features), jnp.bfloat16),
        ),
        in_specs=[SMEM, VMEM, VMEM],
        out_specs=(VMEM, VMEM),
        compiler_params=pltpu.CompilerParams(vmem_limit_bytes=4 * 2**20),
        cost_estimate=cost(rows * features),
        name="fold",
    )(me, keep, got)


def finish_kernel(sizes, scale, *refs):
    chunks = len(sizes)
    keeps, gots = refs[:chunks], refs[chunks : 2 * chunks]
    residual_ref, new_ref, normed_ref = refs[2 * chunks :]
    start = 0
    for chunk, size in enumerate(sizes):
        rows = pl.ds(start, size)
        start += size
        branch = (keeps[chunk][...] + gots[chunk][...].astype(jnp.float32)) * scale
        fresh = (residual_ref[rows, :].astype(jnp.float32) + branch).astype(jnp.bfloat16)
        new_ref[rows, :] = fresh
        values = fresh.astype(jnp.float32)
        inverse = lax.rsqrt(jnp.mean(values * values, axis=1, keepdims=True) + 1e-05)
        normed_ref[rows, :] = (values * inverse).astype(jnp.bfloat16)


def finish(keeps, gots, residual, scale):
    chunks = len(keeps)
    shape = jax.ShapeDtypeStruct(residual.shape, jnp.bfloat16)
    return pl.pallas_call(
        functools.partial(finish_kernel, [keep.shape[0] for keep in keeps], scale),
        out_shape=(shape, shape),
        in_specs=[VMEM] * (2 * chunks + 1),
        out_specs=(VMEM, VMEM),
        compiler_params=pltpu.CompilerParams(vmem_limit_bytes=12 * 2**20),
        cost_estimate=cost(residual.size * 1024),
        name="finish",
    )(*keeps, *gots, residual)


def local(hidden, signs, packed, group_scales, residual):
    groups = lax.axis_size("tensor")
    bits = groups.bit_length() - 1
    me = lax.axis_index("tensor")
    where = me.reshape(1)
    total_width = hidden.shape[1] * groups
    sizes = chunk_rows(residual.shape[0])
    chunks = len(sizes)
    unit = 1.0 / math.sqrt(total_width)
    table = jnp.asarray(dense_table(), jnp.bfloat16)

    def swap(value, bit):
        return lax.ppermute(value, "tensor", [(i, i ^ (1 << bit)) for i in range(groups)])

    def bit_of(bit):
        return jnp.right_shift(me, bit) & 1

    places = [(sum(sizes[:chunk]), sizes[chunk]) for chunk in range(chunks)]
    opened = open_exchange(hidden, signs, groups, sizes[0])
    first, *sent = prepare(hidden, signs, groups, places)
    have = {0: first}
    for bit in reversed(range(bits)):
        wide = bit == bits - 1 and bits > 1
        source = {0: opened} if wide else have
        have.update({r ^ (1 << bit): swap(value, bit) for r, value in list(source.items())})
    stages = [([have[r] for r in range(groups)], table)]
    if chunks > 1:
        other = swap(sent[0], 0)
        pairs = rotate(hidden, signs, other, where, table, groups, places[1:])
        for chunk in range(1, chunks):
            keep, send = pairs[2 * chunk - 2], pairs[2 * chunk - 1]
            for bit in range(1, bits):
                got = swap(send, bit)
                if bit < bits - 1:
                    keep = sign_of(bit_of(bit)) * keep + got.astype(jnp.float32)
                    send = keep.astype(jnp.bfloat16)
            stages.append(([keep, got], None))
    weights = dequantize(packed, group_scales.shape[0])
    words = packed.shape[1]
    side = jnp.arange(group_scales.shape[1]) // words % 2
    scales = group_scales.astype(jnp.float32) * jnp.where(side == 1, 0.0625, 1.0)[None, :]
    scales = scales.astype(jnp.bfloat16)
    keeps, gots = [], []
    for parts, maybe_table in stages:
        value, send = project(parts, where, maybe_table, scales, weights, unit)
        got = swap(send, 0)
        for bit in range(1, bits):
            value, send = fold(value, got, where, bit)
            got = swap(send, bit)
        keeps.append(value)
        gots.append(got)
    return finish(keeps, gots, residual, 1.0 / (45.0 * math.sqrt(total_width)))


def solution(mesh):
    return jax.shard_map(
        local,
        mesh=mesh,
        in_specs=(
            P("dp", "tensor"),
            P("tensor"),
            P("tensor", None),
            P("tensor", None),
            P(("dp", "tensor"), None),
        ),
        out_specs=(P(("dp", "tensor"), None), P(("dp", "tensor"), None)),
        check_vma=False,
    )
```

```python
import functools
import math

import jax
import jax.numpy as jnp
import numpy as np
from jax import lax
from jax.experimental import pallas as pl
from jax.experimental.pallas import tpu as pltpu
from jax.sharding import PartitionSpec as P


ORDER = 28
DENSE = 896
TILE_ROWS = 16
VMEM = pl.BlockSpec(memory_space=pltpu.VMEM)
SMEM = pl.BlockSpec(memory_space=pltpu.SMEM)
HBM = pl.BlockSpec(memory_space=pltpu.HBM)
BYTES = 4
GRANT = 16


def chunk_rows(token_rows):
    quarter = token_rows // 4
    if quarter % TILE_ROWS:
        return [token_rows]
    return [quarter, 2 * quarter, quarter]


def paley_table():
    offsets = (np.arange(13)[None, :] - np.arange(13)[:, None]) % 13
    residues = np.zeros(13)
    residues[np.arange(1, 13) ** 2 % 13] = 1.0
    quadratic = np.where(offsets == 0, 0.0, np.where(residues[offsets] > 0, 1.0, -1.0))
    conference = np.zeros((14, 14))
    conference[0, 1:] = 1.0
    conference[1:, 0] = 1.0
    conference[1:, 1:] = quadratic
    upper = np.array([[1.0, 1.0], [1.0, -1.0]])
    lower = np.array([[1.0, -1.0], [-1.0, -1.0]])
    return np.kron(conference, upper) + np.kron(np.eye(14), lower)


def sylvester(order):
    table = np.ones((1, 1))
    while table.shape[0] < order:
        table = np.kron(np.array([[1.0, 1.0], [1.0, -1.0]]), table)
    return table


def cost(flops):
    return pl.CostEstimate(flops=flops, bytes_accessed=0, transcendentals=0)


def dense_table():
    return np.kron(sylvester(DENSE // ORDER), paley_table().T)


def bit_reversed(groups):
    bits = groups.bit_length() - 1
    return [sum(((d >> b) & 1) << (bits - 1 - b) for b in range(bits)) for d in range(groups)]


def sign_of(bit):
    return (1 - 2 * bit).astype(jnp.float32)


def flips_of(signs):
    return (2 * signs - 1).astype(jnp.float32).reshape(1, signs.shape[0])


def open_kernel(groups, token_rows, size, hidden_ref, signs_ref, out_ref, staged, flips, sems):
    copies = [pltpu.make_async_copy(signs_ref, flips, sems.at[groups])]
    for place, owner in enumerate(bit_reversed(groups)):
        copies.append(
            pltpu.make_async_copy(
                hidden_ref.at[pl.ds(owner * token_rows, size), :],
                staged.at[pl.ds(place * size, size), :],
                sems.at[place],
            )
        )
    for copy in copies:
        copy.start()
    for copy in copies:
        copy.wait()
    out_ref[...] = (staged[...].astype(jnp.float32) * flips_of(flips[...])).astype(jnp.bfloat16)


def open_exchange(hidden, signs, groups, size):
    rows, width = groups * size, hidden.shape[1]
    return pl.pallas_call(
        functools.partial(open_kernel, groups, hidden.shape[0] // groups, size),
        out_shape=jax.ShapeDtypeStruct((rows, width), jnp.bfloat16),
        in_specs=[HBM, HBM],
        out_specs=VMEM,
        scratch_shapes=[
            pltpu.VMEM((rows, width), jnp.bfloat16),
            pltpu.VMEM((width,), jnp.int32),
            pltpu.SemaphoreType.DMA((groups + 1,)),
        ],
        compiler_params=pltpu.CompilerParams(vmem_limit_bytes=8 * 2**20),
        cost_estimate=cost(rows * width),
        name="open_exchange",
    )(*[pltpu.with_memory_space_constraint(value, pltpu.HBM) for value in (hidden, signs)])


def rotate_blocks(mixed, table_ref, stacked_ref):
    rows = mixed[0].shape[0]
    blocks = len(mixed)
    span = 1
    while span < blocks:
        for first in range(blocks):
            if not first & span:
                a, b = mixed[first], mixed[first + span]
                mixed[first], mixed[first + span] = a + b, a - b
        span *= 2
    for block in range(blocks):
        stacked_ref[pl.ds(block * rows, rows), :] = mixed[block].astype(jnp.bfloat16)
    turned = jnp.dot(stacked_ref[...], table_ref[...], preferred_element_type=jnp.float32)
    return [turned[block * rows : (block + 1) * rows] for block in range(blocks)]


def rotate_kernel(groups, places, me_ref, hidden_ref, signs_ref, other_ref, other_signs_ref, table_ref, *refs):
    first_ref, out_refs, stacked_ref = refs[0], refs[1:-1], refs[-1]
    width = hidden_ref.shape[1]
    token_rows = hidden_ref.shape[0] // groups
    flips = flips_of(signs_ref[...]) * sign_of(me_ref[0] & 1)
    other_flips = flips_of(other_signs_ref[...])

    def gather(ref, chosen, columns):
        rows = [
            ref[pl.ds(owner * token_rows + start, size), columns]
            for start, size in chosen
            for owner in bit_reversed(groups)
        ]
        return jnp.concatenate(rows, axis=0).astype(jnp.float32)

    mixed = []
    for block in range(width // DENSE):
        columns = pl.ds(block * DENSE, DENSE)
        flip = flips[:, block * DENSE : (block + 1) * DENSE]
        other_flip = other_flips[:, block * DENSE : (block + 1) * DENSE]
        first = gather(other_ref, places[:1], columns) * other_flip
        first_ref[:, columns] = first.astype(jnp.bfloat16)
        own = gather(hidden_ref, places[1:], columns) * flip
        mixed.append(own + gather(other_ref, places[1:], columns) * other_flip)
    for block, value in enumerate(rotate_blocks(mixed, table_ref, stacked_ref)):
        columns = pl.ds(block * DENSE, DENSE)
        start = 0
        for chunk, (_, size) in enumerate(places[1:]):
            piece = value[start : start + groups * size]
            start += groups * size
            out_refs[2 * chunk][:, columns] = piece
            out_refs[2 * chunk + 1][:, columns] = piece.astype(jnp.bfloat16)


def rotate(hidden, signs, other, other_signs, me, table, groups, places):
    width = hidden.shape[1]
    shapes = [jax.ShapeDtypeStruct((groups * places[0][1], width), jnp.bfloat16)]
    for _, size in places[1:]:
        shapes.append(jax.ShapeDtypeStruct((groups * size, width), jnp.float32))
        shapes.append(jax.ShapeDtypeStruct((groups * size, width), jnp.bfloat16))
    rows = groups * sum(size for _, size in places[1:])
    return pl.pallas_call(
        functools.partial(rotate_kernel, groups, places),
        out_shape=shapes,
        in_specs=[SMEM] + [VMEM] * 5,
        out_specs=[VMEM] * len(shapes),
        scratch_shapes=[pltpu.VMEM((rows * width // DENSE, DENSE), jnp.bfloat16)],
        compiler_params=pltpu.CompilerParams(vmem_limit_bytes=20 * 2**20),
        cost_estimate=cost(2 * rows * width * DENSE),
        name="rotate",
    )(me, hidden, signs, other, other_signs, pltpu.with_memory_space_constraint(table, pltpu.HBM))


def dequantize_kernel(packed_ref, bytes_ref):
    word = packed_ref[...] ^ np.int32(-2139062144)
    for place in range(BYTES):
        moved = jnp.right_shift(jnp.left_shift(word, 24 - 8 * place), 24)
        bytes_ref[place, :, :] = moved.astype(jnp.int8)


def dequantize(packed, group_count):
    width, words = packed.shape
    rows = width // group_count * 7 if group_count % 7 == 0 else width // group_count
    return pl.pallas_call(
        dequantize_kernel,
        grid=(width // rows,),
        out_shape=jax.ShapeDtypeStruct((BYTES, width, words), jnp.int8),
        in_specs=[pl.BlockSpec((rows, words), lambda i: (i, 0))],
        out_specs=pl.BlockSpec((BYTES, rows, words), lambda i: (0, i, 0)),
        compiler_params=pltpu.CompilerParams(vmem_limit_bytes=16 * 2**20),
        cost_estimate=cost(width * words * 8 * 512),
        name="dequantize",
    )(pltpu.with_memory_space_constraint(packed, pltpu.HBM))


def project_kernel(count, unit, rotate_first, me_ref, *refs):
    parts, refs = refs[:count], refs[count:]
    if rotate_first:
        table_ref, refs = refs[0], refs[1:]
    scales_ref, bytes_ref, keep_ref, send_ref, rotated_ref, stacked_ref = refs
    rows, width = parts[0].shape
    words = bytes_ref.shape[2]
    group_count = scales_ref.shape[0]
    group_size = width // group_count
    blocks = width // DENSE
    me = me_ref[0]
    signs = []
    for r in range(count):
        bits = me & (me ^ r) if rotate_first else jnp.right_shift(me, 1) & (1 - r)
        parity = bits & 1
        for shift in range(1, max(count.bit_length() - 1, 1)):
            parity = parity ^ (jnp.right_shift(bits, shift) & 1)
        signs.append(sign_of(parity))
    mixed = []
    for block in range(blocks):
        columns = pl.ds(block * DENSE, DENSE)
        total = signs[0] * parts[0][:, columns].astype(jnp.float32)
        for r in range(1, count):
            total = total + signs[r] * parts[r][:, columns].astype(jnp.float32)
        mixed.append(total)
    if rotate_first:
        mixed = rotate_blocks(mixed, table_ref, stacked_ref)
    for block in range(blocks):
        rotated_ref[:, pl.ds(block * DENSE, DENSE)] = (mixed[block] * unit).astype(jnp.bfloat16)
    half = rows // 2
    upper = me & 1 == 1

    @pl.loop(0, BYTES, unroll=2)
    def _(place):
        spans = [
            pl.ds(pl.multiple_of((2 * place + side) * words, words), words) for side in range(2)
        ]
        sides = [[], []]
        for group in range(group_count):
            both = bytes_ref[place, group * group_size : (group + 1) * group_size, :]
            high = (both & jnp.int8(-16)).astype(jnp.bfloat16)
            low = both.astype(jnp.bfloat16) - high - jnp.bfloat16(8)
            sides[0].append(low * scales_ref[group : group + 1, spans[0]])
            sides[1].append(high * scales_ref[group : group + 1, spans[1]])
        for columns, weights in zip(spans, sides):
            product = jnp.dot(
                rotated_ref[...],
                jnp.concatenate(weights, axis=0),
                preferred_element_type=jnp.float32,
            )
            first, second = product[:half], product[half:]
            keep_ref[:, columns] = jnp.where(upper, second, first)
            send_ref[:, columns] = jnp.where(upper, first, second).astype(jnp.bfloat16)


def project(parts, me, table, scales, weights, unit):
    count = len(parts)
    rows, width = parts[0].shape
    features = scales.shape[1]
    tables = [] if table is None else [table]
    return pl.pallas_call(
        functools.partial(project_kernel, count, unit, table is not None),
        out_shape=(
            jax.ShapeDtypeStruct((rows // 2, features), jnp.float32),
            jax.ShapeDtypeStruct((rows // 2, features), jnp.bfloat16),
        ),
        in_specs=[SMEM] + [VMEM] * (count + len(tables) + 2),
        out_specs=(VMEM, VMEM),
        scratch_shapes=[
            pltpu.VMEM((rows, width), jnp.bfloat16),
            pltpu.VMEM((rows * width // DENSE, DENSE), jnp.bfloat16),
        ],
        compiler_params=pltpu.CompilerParams(vmem_limit_bytes=GRANT * 2**20),
        cost_estimate=cost(2 * 128 * width * features),
        name="project",
    )(me, *parts, *tables, scales, weights)


def fold_kernel(bit, me_ref, keep_ref, got_ref, value_ref, send_ref):
    half = value_ref.shape[0]
    upper = jnp.right_shift(me_ref[0], bit) & 1 == 1
    first = keep_ref[:half, :] + got_ref[:half, :].astype(jnp.float32)
    second = keep_ref[half:, :] + got_ref[half:, :].astype(jnp.float32)
    value_ref[...] = jnp.where(upper, second, first)
    send_ref[...] = jnp.where(upper, first, second).astype(jnp.bfloat16)


def fold(keep, got, me, bit):
    rows, features = keep.shape
    return pl.pallas_call(
        functools.partial(fold_kernel, bit),
        out_shape=(
            jax.ShapeDtypeStruct((rows // 2, features), jnp.float32),
            jax.ShapeDtypeStruct((rows // 2, features), jnp.bfloat16),
        ),
        in_specs=[SMEM, VMEM, VMEM],
        out_specs=(VMEM, VMEM),
        compiler_params=pltpu.CompilerParams(vmem_limit_bytes=4 * 2**20),
        cost_estimate=cost(rows * features),
        name="fold",
    )(me, keep, got)


def finish_kernel(sizes, scale, *refs):
    chunks = len(sizes)
    keeps, gots = refs[:chunks], refs[chunks : 2 * chunks]
    residual_ref, new_ref, normed_ref = refs[2 * chunks :]
    start = 0
    for chunk, size in enumerate(sizes):
        rows = pl.ds(start, size)
        start += size
        branch = (keeps[chunk][...] + gots[chunk][...].astype(jnp.float32)) * scale
        fresh = (residual_ref[rows, :].astype(jnp.float32) + branch).astype(jnp.bfloat16)
        new_ref[rows, :] = fresh
        values = fresh.astype(jnp.float32)
        inverse = lax.rsqrt(jnp.mean(values * values, axis=1, keepdims=True) + 1e-05)
        normed_ref[rows, :] = (values * inverse).astype(jnp.bfloat16)


def finish(keeps, gots, residual, scale):
    chunks = len(keeps)
    shape = jax.ShapeDtypeStruct(residual.shape, jnp.bfloat16)
    return pl.pallas_call(
        functools.partial(finish_kernel, [keep.shape[0] for keep in keeps], scale),
        out_shape=(shape, shape),
        in_specs=[VMEM] * (2 * chunks + 1),
        out_specs=(VMEM, VMEM),
        compiler_params=pltpu.CompilerParams(vmem_limit_bytes=12 * 2**20),
        cost_estimate=cost(residual.size * 1024),
        name="finish",
    )(*keeps, *gots, residual)


def local(hidden, signs, packed, group_scales, residual):
    groups = lax.axis_size("tensor")
    bits = groups.bit_length() - 1
    me = lax.axis_index("tensor")
    where = me.reshape(1)
    total_width = hidden.shape[1] * groups
    sizes = chunk_rows(residual.shape[0])
    chunks = len(sizes)
    unit = 1.0 / math.sqrt(total_width)
    table = jnp.asarray(dense_table(), jnp.bfloat16)

    def swap(value, bit):
        return lax.ppermute(value, "tensor", [(i, i ^ (1 << bit)) for i in range(groups)])

    def bit_of(bit):
        return jnp.right_shift(me, bit) & 1

    places = [(sum(sizes[:chunk]), sizes[chunk]) for chunk in range(chunks)]
    opened = open_exchange(hidden, signs, groups, sizes[0])
    have = {0: opened}
    for bit in reversed(range(1, bits)):
        have.update({r ^ (1 << bit): swap(value, bit) for r, value in list(have.items())})
    if chunks == 1:
        have.update({r ^ 1: swap(value, 0) for r, value in list(have.items())})
        pairs = []
    else:
        other = swap(hidden, 0)
        other_signs = swap(signs, 0)
        first, *pairs = rotate(hidden, signs, other, other_signs, where, table, groups, places)
        have.update({r ^ 1: swap(value, 0) for r, value in list(have.items()) if r})
        have[1] = first
    stages = [([have[r] for r in range(groups)], table)]
    for chunk in range(1, chunks):
        keep, send = pairs[2 * chunk - 2], pairs[2 * chunk - 1]
        for bit in range(1, bits):
            got = swap(send, bit)
            if bit < bits - 1:
                keep = sign_of(bit_of(bit)) * keep + got.astype(jnp.float32)
                send = keep.astype(jnp.bfloat16)
        stages.append(([keep, got], None))
    weights = dequantize(packed, group_scales.shape[0])
    words = packed.shape[1]
    side = jnp.arange(group_scales.shape[1]) // words % 2
    scales = group_scales.astype(jnp.float32) * jnp.where(side == 1, 0.0625, 1.0)[None, :]
    scales = scales.astype(jnp.bfloat16)
    keeps, gots = [], []
    for parts, maybe_table in stages:
        value, send = project(parts, where, maybe_table, scales, weights, unit)
        got = swap(send, 0)
        for bit in range(1, bits):
            value, send = fold(value, got, where, bit)
            got = swap(send, bit)
        keeps.append(value)
        gots.append(got)
    return finish(keeps, gots, residual, 1.0 / (45.0 * math.sqrt(total_width)))


def solution(mesh):
    return jax.shard_map(
        local,
        mesh=mesh,
        in_specs=(
            P("dp", "tensor"),
            P("tensor"),
            P("tensor", None),
            P("tensor", None),
            P(("dp", "tensor"), None),
        ),
        out_specs=(P(("dp", "tensor"), None), P(("dp", "tensor"), None)),
        check_vma=False,
    )
```

```python
import functools
import math

import jax
import jax.numpy as jnp
import numpy as np
from jax import lax
from jax.experimental import pallas as pl
from jax.experimental.pallas import tpu as pltpu
from jax.sharding import PartitionSpec as P


ORDER = 28
DENSE = 896
TILE_ROWS = 16
VMEM = pl.BlockSpec(memory_space=pltpu.VMEM)
SMEM = pl.BlockSpec(memory_space=pltpu.SMEM)
HBM = pl.BlockSpec(memory_space=pltpu.HBM)
BYTES = 4
GRANT = 16


def chunk_rows(token_rows):
    quarter = token_rows // 4
    if quarter % TILE_ROWS:
        return [token_rows]
    return [quarter, 2 * quarter, quarter]


def paley_table():
    offsets = (np.arange(13)[None, :] - np.arange(13)[:, None]) % 13
    residues = np.zeros(13)
    residues[np.arange(1, 13) ** 2 % 13] = 1.0
    quadratic = np.where(offsets == 0, 0.0, np.where(residues[offsets] > 0, 1.0, -1.0))
    conference = np.zeros((14, 14))
    conference[0, 1:] = 1.0
    conference[1:, 0] = 1.0
    conference[1:, 1:] = quadratic
    upper = np.array([[1.0, 1.0], [1.0, -1.0]])
    lower = np.array([[1.0, -1.0], [-1.0, -1.0]])
    return np.kron(conference, upper) + np.kron(np.eye(14), lower)


def sylvester(order):
    table = np.ones((1, 1))
    while table.shape[0] < order:
        table = np.kron(np.array([[1.0, 1.0], [1.0, -1.0]]), table)
    return table


def cost(flops):
    return pl.CostEstimate(flops=flops, bytes_accessed=0, transcendentals=0)


def dense_table():
    return np.kron(sylvester(DENSE // ORDER), paley_table().T)


def bit_reversed(groups):
    bits = groups.bit_length() - 1
    return [sum(((d >> b) & 1) << (bits - 1 - b) for b in range(bits)) for d in range(groups)]


def sign_of(bit):
    return (1 - 2 * bit).astype(jnp.float32)


def flips_of(signs):
    return (2 * signs - 1).astype(jnp.float32).reshape(1, signs.shape[0])


def open_kernel(groups, token_rows, size, hidden_ref, signs_ref, out_ref, staged, flips, sems):
    copies = [pltpu.make_async_copy(signs_ref, flips, sems.at[groups])]
    for place, owner in enumerate(bit_reversed(groups)):
        copies.append(
            pltpu.make_async_copy(
                hidden_ref.at[pl.ds(owner * token_rows, size), :],
                staged.at[pl.ds(place * size, size), :],
                sems.at[place],
            )
        )
    for copy in copies:
        copy.start()
    for copy in copies:
        copy.wait()
    out_ref[...] = (staged[...].astype(jnp.float32) * flips_of(flips[...])).astype(jnp.bfloat16)


def open_exchange(hidden, signs, groups, size):
    rows, width = groups * size, hidden.shape[1]
    return pl.pallas_call(
        functools.partial(open_kernel, groups, hidden.shape[0] // groups, size),
        out_shape=jax.ShapeDtypeStruct((rows, width), jnp.bfloat16),
        in_specs=[HBM, HBM],
        out_specs=VMEM,
        scratch_shapes=[
            pltpu.VMEM((rows, width), jnp.bfloat16),
            pltpu.VMEM((width,), jnp.int32),
            pltpu.SemaphoreType.DMA((groups + 1,)),
        ],
        compiler_params=pltpu.CompilerParams(vmem_limit_bytes=8 * 2**20),
        cost_estimate=cost(rows * width),
        name="open_exchange",
    )(*[pltpu.with_memory_space_constraint(value, pltpu.HBM) for value in (hidden, signs)])


def rotate_blocks(mixed, table_ref, stacked_ref):
    rows = mixed[0].shape[0]
    blocks = len(mixed)
    span = 1
    while span < blocks:
        for first in range(blocks):
            if not first & span:
                a, b = mixed[first], mixed[first + span]
                mixed[first], mixed[first + span] = a + b, a - b
        span *= 2
    for block in range(blocks):
        stacked_ref[pl.ds(block * rows, rows), :] = mixed[block].astype(jnp.bfloat16)
    turned = jnp.dot(stacked_ref[...], table_ref[...], preferred_element_type=jnp.float32)
    return [turned[block * rows : (block + 1) * rows] for block in range(blocks)]


def rotate_kernel(groups, places, me_ref, hidden_ref, signs_ref, other_ref, other_signs_ref, table_ref, *refs):
    first_ref, out_refs, stacked_ref = refs[0], refs[1:-1], refs[-1]
    width = hidden_ref.shape[1]
    token_rows = hidden_ref.shape[0] // groups
    flips = flips_of(signs_ref[...]) * sign_of(me_ref[0] & 1)
    other_flips = flips_of(other_signs_ref[...])

    def gather(ref, chosen, columns):
        rows = [
            ref[pl.ds(owner * token_rows + start, size), columns]
            for start, size in chosen
            for owner in bit_reversed(groups)
        ]
        return jnp.concatenate(rows, axis=0).astype(jnp.float32)

    mixed = []
    for block in range(width // DENSE):
        columns = pl.ds(block * DENSE, DENSE)
        flip = flips[:, block * DENSE : (block + 1) * DENSE]
        other_flip = other_flips[:, block * DENSE : (block + 1) * DENSE]
        first = gather(other_ref, places[:1], columns) * other_flip
        first_ref[:, columns] = first.astype(jnp.bfloat16)
        own = gather(hidden_ref, places[1:], columns) * flip
        mixed.append(own + gather(other_ref, places[1:], columns) * other_flip)
    for block, value in enumerate(rotate_blocks(mixed, table_ref, stacked_ref)):
        columns = pl.ds(block * DENSE, DENSE)
        start = 0
        for chunk, (_, size) in enumerate(places[1:]):
            piece = value[start : start + groups * size]
            start += groups * size
            out_refs[2 * chunk][:, columns] = piece
            out_refs[2 * chunk + 1][:, columns] = piece.astype(jnp.bfloat16)


def rotate(hidden, signs, other, other_signs, me, table, groups, places):
    width = hidden.shape[1]
    shapes = [jax.ShapeDtypeStruct((groups * places[0][1], width), jnp.bfloat16)]
    for _, size in places[1:]:
        shapes.append(jax.ShapeDtypeStruct((groups * size, width), jnp.float32))
        shapes.append(jax.ShapeDtypeStruct((groups * size, width), jnp.bfloat16))
    rows = groups * sum(size for _, size in places[1:])
    return pl.pallas_call(
        functools.partial(rotate_kernel, groups, places),
        out_shape=shapes,
        in_specs=[SMEM] + [VMEM] * 5,
        out_specs=[VMEM] * len(shapes),
        scratch_shapes=[pltpu.VMEM((rows * width // DENSE, DENSE), jnp.bfloat16)],
        compiler_params=pltpu.CompilerParams(vmem_limit_bytes=20 * 2**20),
        cost_estimate=cost(2 * rows * width * DENSE),
        name="rotate",
    )(me, hidden, signs, other, other_signs, pltpu.with_memory_space_constraint(table, pltpu.HBM))


def dequantize_kernel(packed_ref, bytes_ref):
    word = packed_ref[...] ^ np.int32(-2139062144)
    for place in range(BYTES):
        moved = jnp.right_shift(jnp.left_shift(word, 24 - 8 * place), 24)
        bytes_ref[place, :, :] = moved.astype(jnp.int8)


def dequantize(packed, group_count):
    width, words = packed.shape
    rows = width // group_count * 7 if group_count % 7 == 0 else width // group_count
    return pl.pallas_call(
        dequantize_kernel,
        grid=(width // rows,),
        out_shape=jax.ShapeDtypeStruct((BYTES, width, words), jnp.int8),
        in_specs=[pl.BlockSpec((rows, words), lambda i: (i, 0))],
        out_specs=pl.BlockSpec((BYTES, rows, words), lambda i: (0, i, 0)),
        compiler_params=pltpu.CompilerParams(vmem_limit_bytes=16 * 2**20),
        cost_estimate=cost(width * words * 8 * 512),
        name="dequantize",
    )(pltpu.with_memory_space_constraint(packed, pltpu.HBM))


def project_kernel(count, unit, rotate_first, me_ref, *refs):
    parts, refs = refs[:count], refs[count:]
    if rotate_first:
        table_ref, refs = refs[0], refs[1:]
    scales_ref, bytes_ref, keep_ref, send_ref, rotated_ref, stacked_ref = refs
    rows, width = parts[0].shape
    words = bytes_ref.shape[2]
    group_count = scales_ref.shape[0]
    group_size = width // group_count
    blocks = width // DENSE
    me = me_ref[0]
    signs = []
    for r in range(count):
        bits = me & (me ^ r) if rotate_first else jnp.right_shift(me, 1) & (1 - r)
        parity = bits & 1
        for shift in range(1, max(count.bit_length() - 1, 1)):
            parity = parity ^ (jnp.right_shift(bits, shift) & 1)
        signs.append(sign_of(parity))
    mixed = []
    for block in range(blocks):
        columns = pl.ds(block * DENSE, DENSE)
        total = signs[0] * parts[0][:, columns].astype(jnp.float32)
        for r in range(1, count):
            total = total + signs[r] * parts[r][:, columns].astype(jnp.float32)
        mixed.append(total)
    if rotate_first:
        mixed = rotate_blocks(mixed, table_ref, stacked_ref)
    for block in range(blocks):
        rotated_ref[:, pl.ds(block * DENSE, DENSE)] = (mixed[block] * unit).astype(jnp.bfloat16)
    half = rows // 2
    upper = me & 1 == 1

    @pl.loop(0, BYTES, unroll=BYTES)
    def _(place):
        spans = [
            pl.ds(pl.multiple_of((2 * place + side) * words, words), words) for side in range(2)
        ]
        sides = [[], []]
        for group in range(group_count):
            both = bytes_ref[place, group * group_size : (group + 1) * group_size, :]
            high = (both & jnp.int8(-16)).astype(jnp.bfloat16)
            low = both.astype(jnp.bfloat16) - high - jnp.bfloat16(8)
            sides[0].append(low * scales_ref[group : group + 1, spans[0]])
            sides[1].append(high * scales_ref[group : group + 1, spans[1]])
        for columns, weights in zip(spans, sides):
            product = jnp.dot(
                rotated_ref[...],
                jnp.concatenate(weights, axis=0),
                preferred_element_type=jnp.float32,
            )
            first, second = product[:half], product[half:]
            keep_ref[:, columns] = jnp.where(upper, second, first)
            send_ref[:, columns] = jnp.where(upper, first, second).astype(jnp.bfloat16)


def project(parts, me, table, scales, weights, unit):
    count = len(parts)
    rows, width = parts[0].shape
    features = scales.shape[1]
    tables = [] if table is None else [table]
    return pl.pallas_call(
        functools.partial(project_kernel, count, unit, table is not None),
        out_shape=(
            jax.ShapeDtypeStruct((rows // 2, features), jnp.float32),
            jax.ShapeDtypeStruct((rows // 2, features), jnp.bfloat16),
        ),
        in_specs=[SMEM] + [VMEM] * (count + len(tables) + 2),
        out_specs=(VMEM, VMEM),
        scratch_shapes=[
            pltpu.VMEM((rows, width), jnp.bfloat16),
            pltpu.VMEM((rows * width // DENSE, DENSE), jnp.bfloat16),
        ],
        compiler_params=pltpu.CompilerParams(vmem_limit_bytes=GRANT * 2**20),
        cost_estimate=cost(2 * 128 * width * features),
        name="project",
    )(me, *parts, *tables, scales, weights)


def fold_kernel(bit, me_ref, keep_ref, got_ref, value_ref, send_ref):
    half = value_ref.shape[0]
    upper = jnp.right_shift(me_ref[0], bit) & 1 == 1
    first = keep_ref[:half, :] + got_ref[:half, :].astype(jnp.float32)
    second = keep_ref[half:, :] + got_ref[half:, :].astype(jnp.float32)
    value_ref[...] = jnp.where(upper, second, first)
    send_ref[...] = jnp.where(upper, first, second).astype(jnp.bfloat16)


def fold(keep, got, me, bit):
    rows, features = keep.shape
    return pl.pallas_call(
        functools.partial(fold_kernel, bit),
        out_shape=(
            jax.ShapeDtypeStruct((rows // 2, features), jnp.float32),
            jax.ShapeDtypeStruct((rows // 2, features), jnp.bfloat16),
        ),
        in_specs=[SMEM, VMEM, VMEM],
        out_specs=(VMEM, VMEM),
        compiler_params=pltpu.CompilerParams(vmem_limit_bytes=4 * 2**20),
        cost_estimate=cost(rows * features),
        name="fold",
    )(me, keep, got)


def finish_kernel(start, sizes, scale, *refs):
    chunks = len(sizes)
    keeps, gots, residual_ref = refs[:chunks], refs[chunks : 2 * chunks], refs[2 * chunks]
    new_ref, normed_ref, new_rows, normed_rows, sems = refs[-5:]
    copies, at = [], 0
    for chunk, size in enumerate(sizes):
        rows, target = pl.ds(at, size), pl.ds(start + at, size)
        branch = (keeps[chunk][...] + gots[chunk][...].astype(jnp.float32)) * scale
        fresh = (residual_ref[target, :].astype(jnp.float32) + branch).astype(jnp.bfloat16)
        new_rows[rows, :] = fresh
        values = fresh.astype(jnp.float32)
        inverse = lax.rsqrt(jnp.mean(values * values, axis=1, keepdims=True) + 1e-05)
        normed_rows[rows, :] = (values * inverse).astype(jnp.bfloat16)
        at += size
    span, target = pl.ds(0, at), pl.ds(start, at)
    copies.append(pltpu.make_async_copy(new_rows.at[span, :], new_ref.at[target, :], sems.at[0]))
    copies.append(
        pltpu.make_async_copy(normed_rows.at[span, :], normed_ref.at[target, :], sems.at[1])
    )
    for copy in copies:
        copy.start()
    for copy in copies:
        copy.wait()


def finish(keeps, gots, residual, scale, start, begun):
    chunks = len(keeps)
    sizes = [keep.shape[0] for keep in keeps]
    features = residual.shape[1]
    shape = pltpu.HBM(residual.shape, jnp.bfloat16)
    return pl.pallas_call(
        functools.partial(finish_kernel, start, sizes, scale),
        out_shape=(shape, shape),
        in_specs=[VMEM] * (2 * chunks + 1) + [HBM] * len(begun),
        out_specs=(HBM, HBM),
        input_output_aliases={2 * chunks + 1 + i: i for i in range(len(begun))},
        scratch_shapes=[
            pltpu.VMEM((sum(sizes), features), jnp.bfloat16),
            pltpu.VMEM((sum(sizes), features), jnp.bfloat16),
            pltpu.SemaphoreType.DMA((2,)),
        ],
        compiler_params=pltpu.CompilerParams(vmem_limit_bytes=8 * 2**20),
        cost_estimate=cost(residual.size * 64),
        name="finish",
    )(*keeps, *gots, residual, *begun)


def local(hidden, signs, packed, group_scales, residual):
    groups = lax.axis_size("tensor")
    bits = groups.bit_length() - 1
    me = lax.axis_index("tensor")
    where = me.reshape(1)
    total_width = hidden.shape[1] * groups
    sizes = chunk_rows(residual.shape[0])
    chunks = len(sizes)
    unit = 1.0 / math.sqrt(total_width)
    table = jnp.asarray(dense_table(), jnp.bfloat16)

    def swap(value, bit):
        return lax.ppermute(value, "tensor", [(i, i ^ (1 << bit)) for i in range(groups)])

    def bit_of(bit):
        return jnp.right_shift(me, bit) & 1

    places = [(sum(sizes[:chunk]), sizes[chunk]) for chunk in range(chunks)]
    opened = open_exchange(hidden, signs, groups, sizes[0])
    have = {0: opened}
    for bit in reversed(range(1, bits)):
        have.update({r ^ (1 << bit): swap(value, bit) for r, value in list(have.items())})
    if chunks == 1:
        have.update({r ^ 1: swap(value, 0) for r, value in list(have.items())})
        pairs = []
    else:
        other = swap(hidden, 0)
        other_signs = swap(signs, 0)
        first, *pairs = rotate(hidden, signs, other, other_signs, where, table, groups, places)
        have.update({r ^ 1: swap(value, 0) for r, value in list(have.items()) if r})
        have[1] = first
    stages = [([have[r] for r in range(groups)], table)]
    for chunk in range(1, chunks):
        keep, send = pairs[2 * chunk - 2], pairs[2 * chunk - 1]
        for bit in range(1, bits):
            got = swap(send, bit)
            if bit < bits - 1:
                keep = sign_of(bit_of(bit)) * keep + got.astype(jnp.float32)
                send = keep.astype(jnp.bfloat16)
        stages.append(([keep, got], None))
    weights = dequantize(packed, group_scales.shape[0])
    words = packed.shape[1]
    side = jnp.arange(group_scales.shape[1]) // words % 2
    scales = group_scales.astype(jnp.float32) * jnp.where(side == 1, 0.0625, 1.0)[None, :]
    scales = scales.astype(jnp.bfloat16)
    keeps, gots = [], []
    for parts, maybe_table in stages:
        value, send = project(parts, where, maybe_table, scales, weights, unit)
        got = swap(send, 0)
        for bit in range(1, bits):
            value, send = fold(value, got, where, bit)
            got = swap(send, bit)
        keeps.append(value)
        gots.append(got)
    scale = 1.0 / (45.0 * math.sqrt(total_width))
    begun = []
    if chunks > 1:
        begun = finish(keeps[:-1], gots[:-1], residual, scale, 0, [])
    begun = finish(keeps[-1:], gots[-1:], residual, scale, sum(sizes[:-1]), begun)
    return tuple(begun)


def solution(mesh):
    return jax.shard_map(
        local,
        mesh=mesh,
        in_specs=(
            P("dp", "tensor"),
            P("tensor"),
            P("tensor", None),
            P("tensor", None),
            P(("dp", "tensor"), None),
        ),
        out_specs=(P(("dp", "tensor"), None), P(("dp", "tensor"), None)),
        check_vma=False,
    )
```
